32 devices in a mesh: samp: 8 (over z, y), gene: 4 (over x, core).
Axes of the slice: x: 2, y: 2, z: 4, core: 2. Of those that a mesh axis runs over, the one named last changes fastest.
Arguments:
- genotypes: int32 [256, 4096], P('samp', 'gene'), may hold values from -2147483648 to 1789569706, as said below
- allele_freq: float32 [4096], P('gene'), may hold values from 0.035 to 0.56
- sample_weight: float32 [16, 256], P(None, 'samp'), may hold values from 0.2 to 2
- residual: float32 [16, 256], P(None, 'samp'), may hold values from -12 to 12
- variant_weight: float32 [4096], P('gene'), may hold values from 0.2 to 4
- block_gene: int32 [32], replicated, may hold values from 0 to 15, as said below
- gene_variants: int32 [16], replicated, may hold values from 1 to 384, as said below
Outputs:
- burden_z: float32 [16], replicated
- skat_z: float32 [16], replicated
The draws below stay inside these ranges and needn't reach their ends.
Inputs may be any that keep to these rules, and one draw needn't show every extreme that they name: Each word holds 16 dosages 0, 1 or 2: bits 2k and 2k+1 of genotypes[i, v] are the dosage of variant slot v in sample (k, i); a dosage 2 in the top field sets the sign bit. `block_gene`: never falling; the blocks come in aligned groups of four, each shared by two consecutive genes, so every gene has 1 to 3 blocks. `gene_variants`: A gene with m blocks has from (m - 1) * 128 + 1 to m * 128 live variants; the slots after them in its last block are padding.
All inputs are finite; a program needn't handle non-finite values.
Results may differ from the reference program's by a relative error of at most 0.0037.
Values sent between devices are 32-bit elements; how exact they have to be, the bound alone decides.
A program may use at most 64 MiB of HBM per device.

```python
import math
import jax
import jax.numpy as jnp
from jax import lax

FIELDS = 16
BLK = 128
ROWS = 256
SAMPLES = 4096
NBLK = 32
VARIANTS = 4096
NGENE = 16


def gene_layout(key):
    base = jax.random.fold_in(key, 11)
    groups = NBLK // 4
    split_at = jax.random.randint(jax.random.fold_in(base, 1), (groups,), 1, 4, dtype=jnp.int32)
    position = jnp.arange(4, dtype=jnp.int32)
    second = (position[None, :] >= split_at[:, None]).astype(jnp.int32)
    block_gene = (2 * jnp.arange(groups, dtype=jnp.int32)[:, None] + second).reshape(NBLK)
    gene_blocks = jnp.stack([split_at, 4 - split_at], axis=1).reshape(NGENE)
    tail_count = jax.random.randint(jax.random.fold_in(base, 2), (NGENE,), 1, BLK + 1, dtype=jnp.int32)
    return (block_gene, (gene_blocks - 1) * BLK + tail_count)


def draw_block_gene(key, part):
    return gene_layout(key)[0]


def draw_gene_variants(key, part):
    return gene_layout(key)[1]


def allele_levels(key):
    base = jax.random.fold_in(jax.random.fold_in(key, 21), 5)
    return jax.random.randint(base, (VARIANTS,), 40, 520, dtype=jnp.int32)


def draw_allele_freq(key, part):
    levels = allele_levels(key).astype(jnp.float32) / 1024.0
    return levels


def draw_genotypes(key, part):
    levels = allele_levels(key)
    base = jax.random.fold_in(key, 21)
    column = jnp.arange(VARIANTS, dtype=jnp.int32)

    def one_field(field_index, packed):
        field_key = jax.random.fold_in(base, field_index + 100)
        dosage = jnp.zeros((ROWS, VARIANTS), jnp.int32)
        for strand in range(2):
            strand_key = jax.random.fold_in(field_key, strand)
            fresh_bits = (jax.random.randint(jax.random.fold_in(strand_key, 1), (ROWS, VARIANTS), 0, 1024, dtype=jnp.int32) < levels[None, :]).astype(jnp.int32)
            restart = jax.random.randint(jax.random.fold_in(strand_key, 2), (ROWS, VARIANTS), 0, 5, dtype=jnp.int32) == 0
            restart = jnp.logical_or(restart, column[None, :] == 0)
            source = lax.cummax(jnp.where(restart, column[None, :], 0), axis=1)
            dosage = dosage + jnp.take_along_axis(fresh_bits, source, axis=1)
        return packed + jnp.left_shift(dosage, 2 * field_index)
    return lax.fori_loop(0, FIELDS, one_field, jnp.zeros((ROWS, VARIANTS), jnp.int32))


def draw_residual(key, part):
    row_index = jnp.arange(ROWS, dtype=jnp.float32)
    spread = 1.0 + row_index / ROWS
    values = jax.random.truncated_normal(key, -6.0, 6.0, (FIELDS, ROWS), jnp.float32)
    return values * spread[None, :]


def shard_levels(key, extent, shards, low, largest):
    gain, own = 1.0, jax.random.fold_in(key, 6)
    for dim, shards_of in shards:
        draws = jnp.exp(jax.random.uniform(jax.random.fold_in(own, dim), (shards_of,), jnp.float32, low / len(shards), largest / len(shards)))
        gain = gain * jnp.repeat(draws, extent[dim] // shards_of).reshape([-1 if axis == dim else 1 for axis in range(len(extent))])
    return gain


def setup_inputs(seed: int = 0) -> dict:
    streams_of = jax.random.split(jax.random.key(seed), 8)
    return {
        "genotypes": draw_genotypes(jax.random.fold_in(streams_of[7], 71), 0),
        "allele_freq": draw_allele_freq(jax.random.fold_in(streams_of[7], 71), 0),
        "sample_weight": jnp.clip(jnp.exp(math.log(2.0) - 2.3025851 * jax.random.uniform(streams_of[2], (FIELDS, ROWS), jnp.float32) ** shard_levels(streams_of[2], (FIELDS, ROWS), ((1, 8),), -0.2, 0.2)), 0.2, 2.0),
        "residual": draw_residual(jax.random.fold_in(streams_of[7], 71), 0),
        "variant_weight": jnp.clip(jnp.exp(math.log(4.0) - 2.9957323 * jax.random.uniform(streams_of[4], (VARIANTS,), jnp.float32) ** shard_levels(streams_of[4], (VARIANTS,), ((0, 4),), -0.2, 0.2)), 0.2, 4.0),
        "block_gene": draw_block_gene(jax.random.fold_in(streams_of[7], 71), 0),
        "gene_variants": draw_gene_variants(jax.random.fold_in(streams_of[7], 71), 0),
    }


def unpack(packed_words, allele_part, root_weight):
    offsets = 2 * jnp.arange(FIELDS, dtype=jnp.int32)
    dosage = jnp.bitwise_and(jnp.right_shift(packed_words[None, :, :], offsets[:, None, None]), 3)
    centered = dosage.astype(jnp.float32) - 2.0 * allele_part[None, None, :]
    return (root_weight[:, :, None] * centered).astype(jnp.bfloat16)

def block_stats(gram_part, scores, effective):
    weighted_score = effective * scores
    burden_sum = lax.optimization_barrier(jnp.sum(weighted_score, axis=1))
    skat_sum = lax.optimization_barrier(jnp.sum(weighted_score * weighted_score, axis=1))
    image = jnp.einsum('buv,bv->bu', gram_part, effective, precision=lax.Precision.HIGHEST)
    burden_var = lax.optimization_barrier(jnp.sum(effective * image, axis=1))
    diagonal = jnp.diagonal(gram_part, axis1=1, axis2=2)
    trace_one = lax.optimization_barrier(jnp.sum(effective * effective * diagonal, axis=1))
    scaled_gram = effective[:, :, None] * gram_part * effective[:, None, :]
    trace_two = lax.optimization_barrier(jnp.sum(scaled_gram * scaled_gram, axis=(1, 2)))
    return jnp.stack([burden_sum, burden_var, skat_sum, trace_one, trace_two])

def reference(genotypes, allele_freq, sample_weight, residual, variant_weight, block_gene, gene_variants):
    root_weight = jnp.sqrt(sample_weight)
    weighted_residual = (root_weight * residual).astype(jnp.bfloat16).reshape(1, FIELDS * ROWS)
    widened_residual = weighted_residual.astype(jnp.float32)
    variance = jnp.sum(sample_weight * residual * residual) / SAMPLES

    def block_terms(block_index):
        packed_words = lax.dynamic_slice_in_dim(genotypes, block_index * BLK, BLK, 1)
        allele_part = lax.dynamic_slice_in_dim(allele_freq, block_index * BLK, BLK, 0)
        scaled = unpack(packed_words, allele_part, root_weight).reshape(FIELDS * ROWS, BLK)
        widened = scaled.astype(jnp.float32)
        gram_part = jnp.dot(widened.T, widened, precision=lax.Precision.HIGHEST)
        score = jnp.dot(widened_residual, widened, precision=lax.Precision.HIGHEST)[0]
        return (gram_part, score)
    block_index = jnp.arange(NBLK, dtype=jnp.int32)
    gram_all, score_all = lax.map(block_terms, block_index)
    first_block = lax.optimization_barrier(jnp.sum((block_gene[None, :] < block_gene[:, None]).astype(jnp.int32), axis=1))
    counted = gene_variants[block_gene]
    column = jnp.arange(BLK, dtype=jnp.int32)
    is_live = (block_index - first_block)[:, None] * BLK + column[None, :] < counted[:, None]
    effective = variant_weight.reshape(NBLK, BLK) * is_live.astype(jnp.float32)
    stats = block_stats(gram_all, score_all, effective)
    member = (block_gene[:, None] == jnp.arange(NGENE, dtype=jnp.int32)[None, :]).astype(jnp.float32)
    totals = jnp.dot(stats, member, precision=lax.Precision.HIGHEST)
    burden_z = totals[0] / jnp.sqrt(variance * totals[1])
    skat_z = (totals[2] - variance * totals[3]) / (variance * jnp.sqrt(2.0 * totals[4]))
    return (burden_z, skat_z)
```

```python
import functools

import jax
import jax.numpy as jnp
from jax import lax
from jax.experimental import pallas as pl
from jax.experimental.pallas import tpu as pltpu
from jax.sharding import PartitionSpec as P

BLK = 128
MESH = pl.DeviceIdType.MESH
STATS = 5
SCORE = 16


def lane_sum(row):
    return jnp.sum(row, axis=1, keepdims=True)


def owner_range(samp_size, local_blocks):
    low = samp_size // 4
    size = max(1, samp_size // 2)
    while local_blocks % size:
        size -= 1
    return low, size


def flip(samp, step):
    peer, bit = samp, 1
    while bit <= step:
        if step & bit:
            peer = peer + bit * (1 - 2 * lax.rem(lax.div(samp, bit), 2))
        bit *= 2
    return peer


def kernel(
    samp_size,
    gene_size,
    owner_low,
    owner_size,
    genotypes_hbm,
    freq_hbm,
    weight_hbm,
    residual_hbm,
    variant_hbm,
    block_gene_hbm,
    counts_hbm,
    both_ref,
    words_in,
    freq_in,
    weight_in,
    residual_in,
    variant_in,
    block_gene_in,
    counts_in,
    tile_out,
    tiles,
    words,
    scaled,
    centers,
    pair_weight,
    row_out,
    rows,
    load_sem,
    send_sem,
    tile_sem,
    word_sem,
    row_send_sem,
    row_sem,
    ready_sem,
    others_sem,
):
    samp = lax.axis_index("samp")
    gene = lax.axis_index("gene")
    me = samp * gene_size + gene
    fields, local_rows = weight_in.shape
    group = BLK // local_rows
    depth = fields // group
    local_blocks = freq_in.shape[0]
    owned = local_blocks // owner_size
    owner_high = owner_low + owner_size
    genes = counts_in.shape[1]
    width = row_out.shape[1]
    owns = jnp.logical_and(samp >= owner_low, samp < owner_high)
    place = samp - owner_low

    loads = [
        pltpu.make_async_copy(source, target, load_sem.at[number])
        for number, (source, target) in enumerate(
            (
                (genotypes_hbm, words_in),
                (weight_hbm, weight_in),
                (residual_hbm, residual_in),
                (freq_hbm, freq_in),
                (variant_hbm, variant_in),
                (block_gene_hbm, block_gene_in),
                (counts_hbm, counts_in),
            )
        )
    ]
    for load in loads:
        load.start()

    def signal(semaphore, samp_to, gene_to):
        pl.semaphore_signal(
            semaphore,
            inc=1,
            device_id={"samp": samp_to, "gene": gene_to},
            device_id_type=MESH,
        )

    barrier = pltpu.get_barrier_semaphore()
    for gene_to in range(gene_size):

        @pl.when(jnp.logical_and(owns, gene_to > gene))
        def _(gene_to=gene_to):
            signal(barrier, samp, gene_to)

    first_to = jnp.where(owns, samp + 1, jnp.maximum(samp + 1, owner_low))
    last_to = jnp.where(owns, samp_size, owner_high)

    @pl.loop(first_to, last_to)
    def _(samp_to):
        for gene_to in range(gene_size):
            signal(barrier, samp_to, gene_to)

    loads[1].wait()
    loads[2].wait()
    own_weight, own_residual = weight_in[...], residual_in[...]
    own_tile = jnp.concatenate(
        [
            jnp.concatenate(
                [part[lanes * depth : (lanes + 1) * depth] for lanes in range(group)], axis=1
            )
            for part in (own_weight, own_residual)
        ],
        axis=0,
    )
    tile_out[...] = own_tile
    tiles[samp] = own_tile

    earlier_owners = jnp.clip(samp - owner_low, 0, owner_size)
    greeted = jnp.where(owns, me, earlier_owners * gene_size)

    @pl.when(greeted > 0)
    def _():
        pl.semaphore_wait(barrier, greeted)

    @pl.when(owns)
    def _():
        @pl.loop(0, samp)
        def _(samp_to):
            signal(ready_sem.at[place], samp_to, gene)

    def tile_copy(owner):
        return pltpu.make_async_remote_copy(
            src_ref=tile_out,
            dst_ref=tiles.at[samp],
            send_sem=send_sem.at[0],
            recv_sem=tile_sem.at[samp],
            device_id={"samp": owner, "gene": gene},
            device_id_type=MESH,
        )

    def word_copy(owner):
        start = pl.multiple_of((owner - owner_low) * (owned * BLK), BLK)
        return pltpu.make_async_remote_copy(
            src_ref=words_in.at[:, pl.ds(start, owned * BLK)],
            dst_ref=words.at[samp],
            send_sem=send_sem.at[1],
            recv_sem=word_sem.at[samp],
            device_id={"samp": owner, "gene": gene},
            device_id_type=MESH,
        )

    earlier = jnp.minimum(samp, owner_high)

    @pl.loop(owner_low, earlier)
    def _(owner):
        tile_copy(owner).start()

    loads[0].wait()

    @pl.loop(owner_low, earlier)
    def _(owner):
        word_copy(owner).start()

    for gene_to in range(gene_size):

        @pl.when(jnp.logical_and(owns, gene_to < gene))
        def _(gene_to=gene_to):
            signal(others_sem, samp, gene_to)

        @pl.when(gene_to != gene)
        def _(gene_to=gene_to):
            @pl.loop(owner_low, earlier)
            def _(samp_to):
                signal(others_sem, samp_to, gene_to)

    @pl.loop(jnp.maximum(samp + 1, owner_low), owner_high)
    def _(owner):
        pl.semaphore_wait(ready_sem.at[owner - owner_low], 1)
        tile_copy(owner).start()
        word_copy(owner).start()

    for load in loads[3:]:
        load.wait()

    @pl.when(owns)
    def _():
        own_start = pl.multiple_of(place * (owned * BLK), BLK)
        words[samp] = words_in[:, pl.ds(own_start, owned * BLK)]
        block_gene = block_gene_in[...].astype(jnp.float32)
        counts = counts_in[...].astype(jnp.float32)
        block_lane = lax.broadcasted_iota(jnp.int32, block_gene.shape, 1)
        gene_lane = lax.broadcasted_iota(jnp.int32, counts.shape, 1).astype(jnp.float32)
        column = lax.broadcasted_iota(jnp.int32, (1, BLK), 1).astype(jnp.float32)
        stat_sub = lax.broadcasted_iota(jnp.int32, (8, width), 0)
        stat_lane = lax.broadcasted_iota(jnp.int32, (8, width), 1) - stat_sub * genes
        effective, places = [], []
        for block in range(owned):
            local_block = place * owned + block
            block_id = gene * local_blocks + local_block
            gene_of = lane_sum(jnp.where(block_lane == block_id, block_gene, 0.0))
            first = lane_sum(jnp.where(block_gene < gene_of, 1.0, 0.0))
            counted = lane_sum(jnp.where(gene_lane == gene_of, counts, 0.0))
            block_float = jnp.zeros((1, 1), jnp.float32) + block_id.astype(jnp.float32)
            live = (block_float - first) * BLK + column < counted
            weights = jnp.where(live, variant_in[pl.ds(local_block, 1), :], 0.0)
            effective.append(weights)
            across = jnp.broadcast_to(weights, (BLK, BLK))
            pair_weight[block] = across * across.T
            center = 2.0 * jnp.broadcast_to(freq_in[pl.ds(local_block, 1), :], (BLK, BLK)).T
            for level in range(depth):
                centers[block, level] = center * float(4**level)
            member = stat_lane.astype(jnp.float32) == gene_of
            places.append(jnp.where(member & (stat_sub < STATS), 1.0, 0.0))

        def add_peer(peer, totals, power):
            @pl.when(peer != samp)
            def _():
                pltpu.make_async_copy(tile_out, tiles.at[peer], tile_sem.at[peer]).wait()

            tile = tiles[peer]
            weight, resid = tile[:depth], tile[depth:]
            root = jnp.sqrt(weight)
            score = root * resid
            power = power + weight * resid * resid

            @pl.when(peer != samp)
            def _():
                landed = words.at[peer]
                pltpu.make_async_copy(landed, landed, word_sem.at[peer]).wait()

            results = []
            for block in range(owned):
                part = words[peer, :, block * BLK : (block + 1) * BLK]
                turned = jnp.concatenate(
                    [lax.shift_right_logical(part, 2 * depth * lanes) for lanes in range(group)],
                    axis=0,
                ).T
                for level in range(depth):
                    dosage = jnp.bitwise_and(turned, 3 << (2 * level)).astype(jnp.float32)
                    scale = root[level : level + 1] * float(4**-level)
                    lanes = slice(level * BLK, (level + 1) * BLK)
                    scaled[block, :BLK, lanes] = (
                        (dosage - centers[block, level]) * scale
                    ).astype(jnp.bfloat16)
                    scaled[block, BLK:, lanes] = jnp.broadcast_to(
                        score[level : level + 1], (SCORE, BLK)
                    ).astype(jnp.bfloat16)
                results.append(
                    totals[block]
                    + lax.dot_general(
                        scaled[block],
                        scaled[block, :BLK],
                        (((1,), (1,)), ((), ())),
                        preferred_element_type=jnp.float32,
                    )
                )
            return tuple(results), power

        totals = tuple(jnp.zeros((BLK + SCORE, BLK), jnp.float32) for _ in range(owned))
        power = jnp.zeros((depth, BLK), jnp.float32)
        if samp_size == 8:
            for step in (0, 1, 2, 3, 6, 7, 4, 5):
                totals, power = add_peer(flip(samp, step), totals, power)
        else:
            totals, power = lax.fori_loop(
                0,
                samp_size,
                lambda step, carry: add_peer(lax.rem(samp + step, samp_size), *carry),
                (totals, power),
            )

        message = jnp.zeros((8, width), jnp.float32)
        diagonal = lax.broadcasted_iota(jnp.int32, (BLK, BLK), 0) == lax.broadcasted_iota(
            jnp.int32, (BLK, BLK), 1
        )
        for block in range(owned):
            total = totals[block]
            weighted = total[:BLK] * pair_weight[block]
            score = effective[block] * total[BLK : BLK + 1]
            sums = [
                score,
                jnp.sum(weighted, axis=0, keepdims=True),
                score * score,
                jnp.sum(jnp.where(diagonal, weighted, 0.0), axis=0, keepdims=True),
                jnp.sum(weighted * weighted, axis=0, keepdims=True),
                jnp.zeros((8 - STATS, BLK), jnp.float32),
            ]
            message = message + lane_sum(jnp.concatenate(sums, axis=0)) * places[block]
        squares = lane_sum(jnp.sum(power, axis=0, keepdims=True))
        lane = lax.broadcasted_iota(jnp.int32, (1, width), 1)
        reports = jnp.logical_and(place == 0, gene == 0).astype(jnp.float32)
        row = jnp.sum(message, axis=0, keepdims=True) + jnp.where(
            lane == STATS * genes, squares * reports, 0.0
        )

        others = (samp_size - 1 - samp) * (gene_size - 1) + gene_size - 1 - gene

        @pl.when(others > 0)
        def _():
            pl.semaphore_wait(others_sem, others)

        row_out[...] = row
        slot = place * gene_size + gene
        rows[slot] = row

        @pl.loop(0, samp_size)
        def _(samp_to):
            for gene_to in range(gene_size):

                @pl.when(jnp.logical_or(samp_to != samp, gene_to != gene))
                def _(gene_to=gene_to):
                    pltpu.make_async_remote_copy(
                        src_ref=row_out,
                        dst_ref=rows.at[slot],
                        send_sem=row_send_sem,
                        recv_sem=row_sem,
                        device_id={"samp": samp_to, "gene": gene_to},
                        device_id_type=MESH,
                    ).start()

    row_count = owner_size * gene_size

    @pl.when(owns)
    def _():
        landed = rows.at[pl.ds(0, row_count - 1)]
        pltpu.make_async_copy(landed, landed, row_sem).wait()

    @pl.when(jnp.logical_not(owns))
    def _():
        pltpu.make_async_copy(rows, rows, row_sem).wait()

    totals = jnp.sum(rows[...], axis=0)
    parts = [totals[:, stat * genes : (stat + 1) * genes] for stat in range(STATS)]
    variance = totals[:, STATS * genes : STATS * genes + 1] / (fields * local_rows * samp_size)
    both_ref[0:1] = parts[0] / jnp.sqrt(variance * parts[1])
    both_ref[1:2] = (parts[2] - variance * parts[3]) / (
        variance * jnp.sqrt(2.0 * parts[4])
    )

    @pl.when(owns)
    def _():
        devices = samp_size * gene_size

        @pl.loop(0, devices - 1)
        def _(_):
            pltpu.make_async_copy(row_out, row_out, row_send_sem).wait()

    @pl.loop(0, jnp.where(owns, owner_size - 1, owner_size))
    def _(_):
        pltpu.make_async_copy(tile_out, tile_out, send_sem.at[0]).wait()
        pltpu.make_async_copy(words.at[0], words.at[0], send_sem.at[1]).wait()


def solution(mesh):
    samp_size, gene_size = mesh.shape["samp"], mesh.shape["gene"]

    def local(
        genotypes, allele_freq, sample_weight, residual, variant_weight, block_gene, gene_variants
    ):
        local_rows, columns = genotypes.shape
        local_blocks = columns // BLK
        fields = sample_weight.shape[0]
        genes = gene_variants.shape[0]
        depth = fields * local_rows // BLK
        width = -(-(STATS * genes + 1) // BLK) * BLK
        owner_low, owner_size = owner_range(samp_size, local_blocks)
        owned = local_blocks // owner_size
        both = pl.pallas_call(
            functools.partial(kernel, samp_size, gene_size, owner_low, owner_size),
            out_shape=pltpu.VMEM((2, genes), jnp.float32),
            in_specs=[pl.BlockSpec(memory_space=pl.ANY)] * 7,
            out_specs=pl.BlockSpec(memory_space=pltpu.VMEM),
            scratch_shapes=[
                pltpu.VMEM((local_rows, columns), jnp.int32),
                pltpu.VMEM((local_blocks, BLK), jnp.float32),
                pltpu.VMEM((fields, local_rows), jnp.float32),
                pltpu.VMEM((fields, local_rows), jnp.float32),
                pltpu.VMEM((local_blocks, BLK), jnp.float32),
                pltpu.VMEM((1, block_gene.shape[0]), jnp.int32),
                pltpu.VMEM((1, genes), jnp.int32),
                pltpu.VMEM((2 * depth, BLK), jnp.float32),
                pltpu.VMEM((samp_size, 2 * depth, BLK), jnp.float32),
                pltpu.VMEM((samp_size, local_rows, owned * BLK), jnp.int32),
                pltpu.VMEM((owned, BLK + SCORE, depth * BLK), jnp.bfloat16),
                pltpu.VMEM((owned, depth, BLK, BLK), jnp.float32),
                pltpu.VMEM((owned, BLK, BLK), jnp.float32),
                pltpu.VMEM((1, width), jnp.float32),
                pltpu.VMEM((owner_size * gene_size, 1, width), jnp.float32),
                pltpu.SemaphoreType.DMA((7,)),
                pltpu.SemaphoreType.DMA((2,)),
                pltpu.SemaphoreType.DMA((samp_size,)),
                pltpu.SemaphoreType.DMA((samp_size,)),
                pltpu.SemaphoreType.DMA,
                pltpu.SemaphoreType.DMA,
                pltpu.SemaphoreType.REGULAR((owner_size,)),
                pltpu.SemaphoreType.REGULAR,
            ],
            compiler_params=pltpu.CompilerParams(collective_id=0, has_side_effects=True),
        )(
            genotypes,
            allele_freq.reshape(local_blocks, BLK),
            sample_weight,
            residual,
            variant_weight.reshape(local_blocks, BLK),
            block_gene.reshape(1, -1),
            gene_variants.reshape(1, -1),
        )
        return both[0], both[1]

    placed = (P("samp", "gene"), P("gene"), P(None, "samp"), P(None, "samp"), P("gene"), P(), P())
    return jax.shard_map(local, mesh=mesh, in_specs=placed, out_specs=(P(), P()), check_vma=False)
```

```python
import functools

import jax
import jax.numpy as jnp
from jax import lax
from jax.experimental import pallas as pl
from jax.experimental.pallas import tpu as pltpu
from jax.sharding import PartitionSpec as P

BLK = 128
MESH = pl.DeviceIdType.MESH
STATS = 5
SCORE = 16


def lane_sum(row):
    return jnp.sum(row, axis=1, keepdims=True)


def owner_range(samp_size, local_blocks):
    low = samp_size // 4
    size = max(1, samp_size // 2)
    while local_blocks % size:
        size -= 1
    return low, size


def flip(samp, step):
    peer, bit = samp, 1
    while bit <= step:
        if step & bit:
            peer = peer + bit * (1 - 2 * lax.rem(lax.div(samp, bit), 2))
        bit *= 2
    return peer


def kernel(
    samp_size,
    gene_size,
    owner_low,
    owner_size,
    genotypes_hbm,
    freq_hbm,
    weight_hbm,
    residual_hbm,
    variant_hbm,
    block_gene_hbm,
    counts_hbm,
    both_ref,
    words_in,
    freq_in,
    weight_in,
    residual_in,
    variant_in,
    block_gene_in,
    counts_in,
    tile_out,
    tiles,
    words,
    scaled,
    centers,
    pair_weight,
    row_out,
    rows,
    load_sem,
    send_sem,
    tile_sem,
    word_sem,
    row_send_sem,
    row_sem,
):
    samp = lax.axis_index("samp")
    gene = lax.axis_index("gene")
    me = samp * gene_size + gene
    fields, local_rows = weight_in.shape
    group = BLK // local_rows
    depth = fields // group
    local_blocks = freq_in.shape[0]
    owned = local_blocks // owner_size
    owner_high = owner_low + owner_size
    genes = counts_in.shape[1]
    width = row_out.shape[1]
    owns = jnp.logical_and(samp >= owner_low, samp < owner_high)
    place = samp - owner_low
    row_count = owner_size * gene_size

    loads = [
        pltpu.make_async_copy(source, target, load_sem.at[number])
        for number, (source, target) in enumerate(
            (
                (genotypes_hbm, words_in),
                (weight_hbm, weight_in),
                (residual_hbm, residual_in),
                (freq_hbm, freq_in),
                (variant_hbm, variant_in),
                (block_gene_hbm, block_gene_in),
                (counts_hbm, counts_in),
            )
        )
    ]
    for load in loads:
        load.start()

    def signal(semaphore, samp_to, gene_to):
        pl.semaphore_signal(
            semaphore,
            inc=1,
            device_id={"samp": samp_to, "gene": gene_to},
            device_id_type=MESH,
        )

    barrier = pltpu.get_barrier_semaphore()

    @pl.when(owns)
    def _():
        @pl.loop(1, samp_size)
        def _(step):
            signal(barrier, lax.rem(samp + step, samp_size), gene)

    for step in range(1, gene_size):
        signal(barrier, samp, lax.rem(gene + step, gene_size))

    loads[1].wait()
    loads[2].wait()
    own_weight, own_residual = weight_in[...], residual_in[...]
    own_tile = jnp.concatenate(
        [
            jnp.concatenate(
                [part[lanes * depth : (lanes + 1) * depth] for lanes in range(group)], axis=1
            )
            for part in (own_weight, own_residual)
        ],
        axis=0,
    )
    tile_out[...] = own_tile
    tiles[samp] = own_tile

    pl.semaphore_wait(barrier, jnp.where(owns, owner_size - 1, owner_size) + gene_size - 1)

    def tile_copy(owner):
        return pltpu.make_async_remote_copy(
            src_ref=tile_out,
            dst_ref=tiles.at[samp],
            send_sem=send_sem.at[0],
            recv_sem=tile_sem.at[samp],
            device_id={"samp": owner, "gene": gene},
            device_id_type=MESH,
        )

    def word_copy(owner):
        start = pl.multiple_of((owner - owner_low) * (owned * BLK), BLK)
        return pltpu.make_async_remote_copy(
            src_ref=words_in.at[:, pl.ds(start, owned * BLK)],
            dst_ref=words.at[samp],
            send_sem=send_sem.at[1],
            recv_sem=word_sem.at[samp],
            device_id={"samp": owner, "gene": gene},
            device_id_type=MESH,
        )

    upward = 2 * samp < 2 * owner_low + owner_size

    def to_owners(send):
        for order in range(owner_size):
            owner = jnp.where(upward, owner_high - 1 - order, owner_low + order)

            @pl.when(owner != samp)
            def _(owner=owner):
                send(owner).start()

    to_owners(tile_copy)
    loads[0].wait()
    to_owners(word_copy)

    for load in loads[3:]:
        load.wait()

    @pl.when(owns)
    def _():
        own_start = pl.multiple_of(place * (owned * BLK), BLK)
        words[samp] = words_in[:, pl.ds(own_start, owned * BLK)]
        block_gene = block_gene_in[...].astype(jnp.float32)
        counts = counts_in[...].astype(jnp.float32)
        block_lane = lax.broadcasted_iota(jnp.int32, block_gene.shape, 1)
        gene_lane = lax.broadcasted_iota(jnp.int32, counts.shape, 1).astype(jnp.float32)
        column = lax.broadcasted_iota(jnp.int32, (1, BLK), 1).astype(jnp.float32)
        stat_sub = lax.broadcasted_iota(jnp.int32, (8, width), 0)
        stat_lane = lax.broadcasted_iota(jnp.int32, (8, width), 1) - stat_sub * genes
        effective, places = [], []
        for block in range(owned):
            local_block = place * owned + block
            block_id = gene * local_blocks + local_block
            gene_of = lane_sum(jnp.where(block_lane == block_id, block_gene, 0.0))
            first = lane_sum(jnp.where(block_gene < gene_of, 1.0, 0.0))
            counted = lane_sum(jnp.where(gene_lane == gene_of, counts, 0.0))
            block_float = jnp.zeros((1, 1), jnp.float32) + block_id.astype(jnp.float32)
            live = (block_float - first) * BLK + column < counted
            weights = jnp.where(live, variant_in[pl.ds(local_block, 1), :], 0.0)
            effective.append(weights)
            across = jnp.broadcast_to(weights, (BLK, BLK))
            pair_weight[block] = across * across.T
            center = 2.0 * jnp.broadcast_to(freq_in[pl.ds(local_block, 1), :], (BLK, BLK)).T
            for level in range(depth):
                centers[block, level] = center * float(4**level)
            member = stat_lane.astype(jnp.float32) == gene_of
            places.append(jnp.where(member & (stat_sub < STATS), 1.0, 0.0))

        def add_peer(peer, totals, power):
            @pl.when(peer != samp)
            def _():
                pltpu.make_async_copy(tile_out, tiles.at[peer], tile_sem.at[peer]).wait()

            tile = tiles[peer]
            weight, resid = tile[:depth], tile[depth:]
            root = jnp.sqrt(weight)
            score = root * resid
            power = power + weight * resid * resid

            @pl.when(peer != samp)
            def _():
                landed = words.at[peer]
                pltpu.make_async_copy(landed, landed, word_sem.at[peer]).wait()

            results = []
            for block in range(owned):
                part = words[peer, :, block * BLK : (block + 1) * BLK]
                turned = jnp.concatenate(
                    [lax.shift_right_logical(part, 2 * depth * lanes) for lanes in range(group)],
                    axis=0,
                ).T
                for level in range(depth):
                    dosage = jnp.bitwise_and(turned, 3 << (2 * level)).astype(jnp.float32)
                    scale = root[level : level + 1] * float(4**-level)
                    lanes = slice(level * BLK, (level + 1) * BLK)
                    scaled[block, :BLK, lanes] = (
                        (dosage - centers[block, level]) * scale
                    ).astype(jnp.bfloat16)
                    scaled[block, BLK:, lanes] = jnp.broadcast_to(
                        score[level : level + 1], (SCORE, BLK)
                    ).astype(jnp.bfloat16)
                results.append(
                    totals[block]
                    + lax.dot_general(
                        scaled[block],
                        scaled[block, :BLK],
                        (((1,), (1,)), ((), ())),
                        preferred_element_type=jnp.float32,
                    )
                )
            return tuple(results), power

        totals = tuple(jnp.zeros((BLK + SCORE, BLK), jnp.float32) for _ in range(owned))
        power = jnp.zeros((depth, BLK), jnp.float32)
        if samp_size == 8:
            for step in (0, 1, 6, 7, 4, 5, 2, 3):
                totals, power = add_peer(flip(samp, step), totals, power)
        else:
            totals, power = lax.fori_loop(
                0,
                samp_size,
                lambda step, carry: add_peer(lax.rem(samp + step, samp_size), *carry),
                (totals, power),
            )

        message = jnp.zeros((8, width), jnp.float32)
        diagonal = lax.broadcasted_iota(jnp.int32, (BLK, BLK), 0) == lax.broadcasted_iota(
            jnp.int32, (BLK, BLK), 1
        )
        for block in range(owned):
            total = totals[block]
            weighted = total[:BLK] * pair_weight[block]
            score = effective[block] * total[BLK : BLK + 1]
            sums = [
                score,
                jnp.sum(weighted, axis=0, keepdims=True),
                score * score,
                jnp.sum(jnp.where(diagonal, weighted, 0.0), axis=0, keepdims=True),
                jnp.sum(weighted * weighted, axis=0, keepdims=True),
                jnp.zeros((8 - STATS, BLK), jnp.float32),
            ]
            message = message + lane_sum(jnp.concatenate(sums, axis=0)) * places[block]
        squares = lane_sum(jnp.sum(power, axis=0, keepdims=True))
        lane = lax.broadcasted_iota(jnp.int32, (1, width), 1)
        reports = jnp.logical_and(place == 0, gene == 0).astype(jnp.float32)
        row = jnp.sum(message, axis=0, keepdims=True) + jnp.where(
            lane == STATS * genes, squares * reports, 0.0
        )

        row_out[...] = row
        slot = place * gene_size + gene
        rows[slot] = row

        @pl.loop(0, samp_size)
        def _(samp_to):
            for gene_to in range(gene_size):

                @pl.when(jnp.logical_or(samp_to != samp, gene_to != gene))
                def _(gene_to=gene_to):
                    pltpu.make_async_remote_copy(
                        src_ref=row_out,
                        dst_ref=rows.at[slot],
                        send_sem=row_send_sem,
                        recv_sem=row_sem,
                        device_id={"samp": samp_to, "gene": gene_to},
                        device_id_type=MESH,
                    ).start()

    @pl.when(owns)
    def _():
        landed = rows.at[pl.ds(0, row_count - 1)]
        pltpu.make_async_copy(landed, landed, row_sem).wait()

    @pl.when(jnp.logical_not(owns))
    def _():
        pltpu.make_async_copy(rows, rows, row_sem).wait()

    totals = jnp.sum(rows[...], axis=0)
    parts = [totals[:, stat * genes : (stat + 1) * genes] for stat in range(STATS)]
    variance = totals[:, STATS * genes : STATS * genes + 1] / (fields * local_rows * samp_size)
    both_ref[0:1] = parts[0] / jnp.sqrt(variance * parts[1])
    both_ref[1:2] = (parts[2] - variance * parts[3]) / (
        variance * jnp.sqrt(2.0 * parts[4])
    )

    @pl.when(owns)
    def _():
        devices = samp_size * gene_size

        @pl.loop(0, devices - 1)
        def _(_):
            pltpu.make_async_copy(row_out, row_out, row_send_sem).wait()

    @pl.loop(0, jnp.where(owns, owner_size - 1, owner_size))
    def _(_):
        pltpu.make_async_copy(tile_out, tile_out, send_sem.at[0]).wait()
        pltpu.make_async_copy(words.at[0], words.at[0], send_sem.at[1]).wait()


def solution(mesh):
    samp_size, gene_size = mesh.shape["samp"], mesh.shape["gene"]

    def local(
        genotypes, allele_freq, sample_weight, residual, variant_weight, block_gene, gene_variants
    ):
        local_rows, columns = genotypes.shape
        local_blocks = columns // BLK
        fields = sample_weight.shape[0]
        genes = gene_variants.shape[0]
        depth = fields * local_rows // BLK
        width = -(-(STATS * genes + 1) // BLK) * BLK
        owner_low, owner_size = owner_range(samp_size, local_blocks)
        owned = local_blocks // owner_size
        both = pl.pallas_call(
            functools.partial(kernel, samp_size, gene_size, owner_low, owner_size),
            out_shape=pltpu.VMEM((2, genes), jnp.float32),
            in_specs=[pl.BlockSpec(memory_space=pl.ANY)] * 7,
            out_specs=pl.BlockSpec(memory_space=pltpu.VMEM),
            scratch_shapes=[
                pltpu.VMEM((local_rows, columns), jnp.int32),
                pltpu.VMEM((local_blocks, BLK), jnp.float32),
                pltpu.VMEM((fields, local_rows), jnp.float32),
                pltpu.VMEM((fields, local_rows), jnp.float32),
                pltpu.VMEM((local_blocks, BLK), jnp.float32),
                pltpu.VMEM((1, block_gene.shape[0]), jnp.int32),
                pltpu.VMEM((1, genes), jnp.int32),
                pltpu.VMEM((2 * depth, BLK), jnp.float32),
                pltpu.VMEM((samp_size, 2 * depth, BLK), jnp.float32),
                pltpu.VMEM((samp_size, local_rows, owned * BLK), jnp.int32),
                pltpu.VMEM((owned, BLK + SCORE, depth * BLK), jnp.bfloat16),
                pltpu.VMEM((owned, depth, BLK, BLK), jnp.float32),
                pltpu.VMEM((owned, BLK, BLK), jnp.float32),
                pltpu.VMEM((1, width), jnp.float32),
                pltpu.VMEM((owner_size * gene_size, 1, width), jnp.float32),
                pltpu.SemaphoreType.DMA((7,)),
                pltpu.SemaphoreType.DMA((2,)),
                pltpu.SemaphoreType.DMA((samp_size,)),
                pltpu.SemaphoreType.DMA((samp_size,)),
                pltpu.SemaphoreType.DMA,
                pltpu.SemaphoreType.DMA,
            ],
            compiler_params=pltpu.CompilerParams(collective_id=0, has_side_effects=True),
        )(
            genotypes,
            allele_freq.reshape(local_blocks, BLK),
            sample_weight,
            residual,
            variant_weight.reshape(local_blocks, BLK),
            block_gene.reshape(1, -1),
            gene_variants.reshape(1, -1),
        )
        return both[0], both[1]

    placed = (P("samp", "gene"), P("gene"), P(None, "samp"), P(None, "samp"), P("gene"), P(), P())
    return jax.shard_map(local, mesh=mesh, in_specs=placed, out_specs=(P(), P()), check_vma=False)
```

```python
import functools

import jax
import jax.numpy as jnp
from jax import lax
from jax.experimental import pallas as pl
from jax.experimental.pallas import tpu as pltpu
from jax.sharding import PartitionSpec as P

BLK = 128
MESH = pl.DeviceIdType.MESH
STATS = 5
SCORE = 16
PAIR = 2
CHUNK = 2
ORDER = ((1, 0), (1, 3), (0, 0), (0, 3), (1, 2), (1, 1), (0, 2), (0, 1))


def lane_sum(row):
    return jnp.sum(row, axis=1, keepdims=True)


def owner_range(samp_size, local_blocks):
    low = samp_size // 4
    size = max(1, samp_size // 2)
    while local_blocks % size:
        size -= 1
    return low, size


def flip(samp, step):
    peer, bit = samp, 1
    while bit <= step:
        if step & bit:
            peer = peer + bit * (1 - 2 * lax.rem(lax.div(samp, bit), 2))
        bit *= 2
    return peer


def kernel(
    samp_size,
    gene_size,
    owner_low,
    owner_size,
    genotypes_hbm,
    freq_hbm,
    weight_hbm,
    residual_hbm,
    variant_hbm,
    block_gene_hbm,
    counts_hbm,
    both_ref,
    words_in,
    weight_in,
    residual_in,
    block_gene_in,
    counts_in,
    params,
    tile_out,
    tiles,
    words,
    centers,
    pair_weight,
    row_out,
    rows,
    load_sem,
    send_sem,
    tile_sem,
    word_sem,
    param_sem,
    row_sem,
):
    samp = lax.axis_index("samp")
    gene = lax.axis_index("gene")
    side = lax.rem(gene, PAIR)
    lead = gene - side + (PAIR - 1)
    fields, local_rows = weight_in.shape
    group = BLK // local_rows
    depth = fields // group
    local_blocks = params.shape[2]
    owned = local_blocks // owner_size
    owner_high = owner_low + owner_size
    genes = counts_in.shape[1]
    width = row_out.shape[1]
    leads = side == PAIR - 1
    in_range = jnp.logical_and(samp >= owner_low, samp < owner_high)
    owns = jnp.logical_and(leads, in_range)
    helps = jnp.logical_and(jnp.logical_not(leads), in_range)
    place = samp - owner_low
    pairs = gene_size // PAIR
    row_count = owner_size * pairs

    loads = [
        pltpu.make_async_copy(source, target, load_sem.at[number])
        for number, source, target in (
            (0, genotypes_hbm, words_in),
            (1, weight_hbm, weight_in),
            (1, residual_hbm, residual_in),
            (2, freq_hbm, params.at[side, 0]),
            (2, variant_hbm, params.at[side, 1]),
            (2, block_gene_hbm, block_gene_in),
            (2, counts_hbm, counts_in),
        )
    ]
    for load in loads[1:] + loads[:1]:
        load.start()

    def signal(semaphore, samp_to, gene_to):
        pl.semaphore_signal(
            semaphore,
            inc=1,
            device_id={"samp": samp_to, "gene": gene_to},
            device_id_type=MESH,
        )

    barrier = pltpu.get_barrier_semaphore()

    @pl.when(owns)
    def _():
        for other in range(1, PAIR):
            signal(barrier, samp, gene - other)

        @pl.loop(1, samp_size)
        def _(step):
            for other in range(PAIR):
                signal(barrier, lax.rem(samp + step, samp_size), gene - other)

    for step in range(1, pairs):
        signal(barrier, samp, lax.rem(gene + step * PAIR, gene_size))

    loads[1].wait()
    loads[2].wait()
    own_tile = jnp.concatenate(
        [
            jnp.concatenate(
                [part[lanes * depth : (lanes + 1) * depth] for lanes in range(group)], axis=1
            )
            for part in (weight_in[...], residual_in[...])
        ],
        axis=0,
    )
    tile_out[...] = own_tile
    tiles[samp] = own_tile

    pl.semaphore_wait(barrier, jnp.where(owns, owner_size - 1, owner_size) + pairs - 1)

    chunk = lax.div(samp, CHUNK)

    def tile_copy(owner):
        return pltpu.make_async_remote_copy(
            src_ref=tile_out,
            dst_ref=tiles.at[samp],
            send_sem=send_sem,
            recv_sem=tile_sem.at[chunk],
            device_id={"samp": owner, "gene": lead},
            device_id_type=MESH,
        )

    def word_copy(owner):
        start = pl.multiple_of((owner - owner_low) * (owned * BLK), BLK)
        return pltpu.make_async_remote_copy(
            src_ref=words_in.at[:, pl.ds(start, owned * BLK)],
            dst_ref=words.at[side, samp],
            send_sem=send_sem,
            recv_sem=word_sem.at[side, chunk],
            device_id={"samp": owner, "gene": lead},
            device_id_type=MESH,
        )

    upward = 2 * samp < 2 * owner_low + owner_size

    def to_owners(send, condition):
        for order in range(owner_size):
            owner = jnp.where(upward, owner_high - 1 - order, owner_low + order)

            @pl.when(condition(owner))
            def _(owner=owner):
                send(owner).start()

    to_owners(tile_copy, lambda owner: jnp.logical_and(leads, owner != samp))
    loads[0].wait()
    to_owners(
        word_copy, lambda owner: jnp.logical_or(jnp.logical_not(leads), owner != samp)
    )
    for load in loads[3:]:
        load.wait()

    @pl.when(helps)
    def _():
        pltpu.make_async_remote_copy(
            src_ref=params.at[side],
            dst_ref=params.at[side],
            send_sem=send_sem,
            recv_sem=param_sem,
            device_id={"samp": samp, "gene": lead},
            device_id_type=MESH,
        ).start()

    @pl.when(owns)
    def _():
        own_start = pl.multiple_of(place * (owned * BLK), BLK)
        words[PAIR - 1, samp] = words_in[:, pl.ds(own_start, owned * BLK)]
        if PAIR > 1:
            landed = params.at[pl.ds(0, PAIR - 1)]
            pltpu.make_async_copy(landed, landed, param_sem).wait()
        block_gene = block_gene_in[...].astype(jnp.float32)
        counts = counts_in[...].astype(jnp.float32)
        block_lane = lax.broadcasted_iota(jnp.int32, block_gene.shape, 1)
        gene_lane = lax.broadcasted_iota(jnp.int32, counts.shape, 1).astype(jnp.float32)
        column = lax.broadcasted_iota(jnp.int32, (1, BLK), 1).astype(jnp.float32)
        stat_sub = lax.broadcasted_iota(jnp.int32, (8, width), 0)
        stat_lane = lax.broadcasted_iota(jnp.int32, (8, width), 1) - stat_sub * genes
        effective, places = [], []
        for number in range(PAIR * owned):
            from_side, block = divmod(number, owned)
            local_block = place * owned + block
            block_id = (lead - (PAIR - 1) + from_side) * local_blocks + local_block
            gene_of = lane_sum(jnp.where(block_lane == block_id, block_gene, 0.0))
            first = lane_sum(jnp.where(block_gene < gene_of, 1.0, 0.0))
            counted = lane_sum(jnp.where(gene_lane == gene_of, counts, 0.0))
            block_float = jnp.zeros((1, 1), jnp.float32) + block_id.astype(jnp.float32)
            live = (block_float - first) * BLK + column < counted
            weights = jnp.where(live, params[from_side, 1, pl.ds(local_block, 1), :], 0.0)
            effective.append(weights)
            across = jnp.broadcast_to(weights, (BLK, BLK))
            pair_weight[number] = across * across.T
            freq = params[from_side, 0, pl.ds(local_block, 1), :]
            center = 2.0 * jnp.broadcast_to(freq, (BLK, BLK)).T
            for level in range(depth):
                centers[number, level] = center * float(4**level)
            member = stat_lane.astype(jnp.float32) == gene_of
            places.append(jnp.where(member & (stat_sub < STATS), 1.0, 0.0))

        def land(buffer, semaphore):
            pltpu.make_async_copy(buffer, buffer, semaphore).wait()

        def unpack(from_side, peer, power):
            tile = tiles[peer]
            weight, resid = tile[:depth], tile[depth:]
            root = jnp.sqrt(weight)
            score = root * resid
            values = []
            for block in range(owned):
                part = words[from_side, peer, :, block * BLK : (block + 1) * BLK]
                turned = jnp.concatenate(
                    [lax.shift_right_logical(part, 2 * depth * lanes) for lanes in range(group)],
                    axis=0,
                ).T
                levels = []
                for level in range(depth):
                    dosage = jnp.bitwise_and(turned, 3 << (2 * level)).astype(jnp.float32)
                    scale = root[level : level + 1] * float(4**-level)
                    center = centers[from_side * owned + block, level]
                    levels.append(((dosage - center) * scale).astype(jnp.bfloat16))
                values.append(jnp.concatenate(levels, axis=1))
            scores = jnp.concatenate(
                [
                    jnp.broadcast_to(score[level : level + 1], (SCORE, BLK)).astype(jnp.bfloat16)
                    for level in range(depth)
                ],
                axis=1,
            )
            if from_side == PAIR - 1:
                power = power + weight * resid * resid
            return (from_side, values, scores), power

        def multiply(unpacked, totals):
            from_side, values, scores = unpacked
            totals = list(totals)
            for block in range(owned):
                number = from_side * owned + block
                totals[number] = totals[number] + lax.dot_general(
                    jnp.concatenate([values[block], scores], axis=0),
                    values[block],
                    (((1,), (1,)), ((), ())),
                    preferred_element_type=jnp.float32,
                )
            return tuple(totals)

        def wait_chunk(from_side, from_chunk, own):
            first = from_chunk * CHUNK
            if from_side < PAIR - 1:
                land(words.at[from_side, pl.ds(first, CHUNK)], word_sem.at[from_side, from_chunk])
            elif own:
                peer = flip(samp, 1)
                land(tiles.at[peer], tile_sem.at[from_chunk])
                land(words.at[from_side, peer], word_sem.at[from_side, from_chunk])
            else:
                land(tiles.at[pl.ds(first, CHUNK)], tile_sem.at[from_chunk])
                land(words.at[from_side, pl.ds(first, CHUNK)], word_sem.at[from_side, from_chunk])

        chunks = samp_size // CHUNK
        totals = tuple(jnp.zeros((BLK + SCORE, BLK), jnp.float32) for _ in range(PAIR * owned))
        power = jnp.zeros((depth, BLK), jnp.float32)
        if chunks == 4:
            waiting = None
            for from_side, step in ORDER:
                from_chunk = flip(chunk, step)
                wait_chunk(from_side, from_chunk, step == 0)
                for member in range(CHUNK):
                    ahead, power = unpack(from_side, from_chunk * CHUNK + member, power)
                    if waiting is not None:
                        totals = multiply(waiting, totals)
                    waiting = ahead
            totals = multiply(waiting, totals)
        else:

            def add_chunk(from_chunk, totals, power, own):
                for from_side in reversed(range(PAIR)):
                    wait_chunk(from_side, from_chunk, own)
                    for member in range(CHUNK):
                        ahead, power = unpack(from_side, from_chunk * CHUNK + member, power)
                        totals = multiply(ahead, totals)
                return totals, power

            totals, power = lax.fori_loop(
                1,
                chunks,
                lambda step, carry: add_chunk(lax.rem(chunk + step, chunks), *carry, False),
                add_chunk(chunk, totals, power, True),
            )

        message = jnp.zeros((8, width), jnp.float32)
        diagonal = lax.broadcasted_iota(jnp.int32, (BLK, BLK), 0) == lax.broadcasted_iota(
            jnp.int32, (BLK, BLK), 1
        )
        for number in range(PAIR * owned):
            total = totals[number]
            weighted = total[:BLK] * pair_weight[number]
            score = effective[number] * total[BLK : BLK + 1]
            sums = [
                score,
                jnp.sum(weighted, axis=0, keepdims=True),
                score * score,
                jnp.sum(jnp.where(diagonal, weighted, 0.0), axis=0, keepdims=True),
                jnp.sum(weighted * weighted, axis=0, keepdims=True),
                jnp.zeros((8 - STATS, BLK), jnp.float32),
            ]
            message = message + lane_sum(jnp.concatenate(sums, axis=0)) * places[number]
        squares = lane_sum(jnp.sum(power, axis=0, keepdims=True))
        lane = lax.broadcasted_iota(jnp.int32, (1, width), 1)
        reports = jnp.logical_and(place == 0, lead == PAIR - 1).astype(jnp.float32)
        row = jnp.sum(message, axis=0, keepdims=True) + jnp.where(
            lane == STATS * genes, squares * reports, 0.0
        )
        row_out[...] = row
        slot = place * pairs + lax.div(gene, PAIR)
        rows[slot] = row

        @pl.loop(0, samp_size)
        def _(samp_to):
            for gene_to in range(gene_size):

                @pl.when(jnp.logical_or(samp_to != samp, gene_to != gene))
                def _(gene_to=gene_to):
                    pltpu.make_async_remote_copy(
                        src_ref=row_out,
                        dst_ref=rows.at[slot],
                        send_sem=send_sem,
                        recv_sem=row_sem,
                        device_id={"samp": samp_to, "gene": gene_to},
                        device_id_type=MESH,
                    ).start()

    @pl.when(owns)
    def _():
        landed = rows.at[pl.ds(0, row_count - 1)]
        pltpu.make_async_copy(landed, landed, row_sem).wait()

    @pl.when(jnp.logical_not(owns))
    def _():
        pltpu.make_async_copy(rows, rows, row_sem).wait()

    totals = jnp.sum(rows[...], axis=0)
    parts = [totals[:, stat * genes : (stat + 1) * genes] for stat in range(STATS)]
    variance = totals[:, STATS * genes : STATS * genes + 1] / (fields * local_rows * samp_size)
    both_ref[0:1] = parts[0] / jnp.sqrt(variance * parts[1])
    both_ref[1:2] = (parts[2] - variance * parts[3]) / (
        variance * jnp.sqrt(2.0 * parts[4])
    )

    def sent(buffer, count):
        @pl.loop(0, count)
        def _(_):
            pltpu.make_async_copy(buffer, buffer, send_sem).wait()

    targets = jnp.where(owns, owner_size - 1, owner_size)
    sent(words.at[0, 0], targets)
    sent(tile_out, jnp.where(leads, targets, 0))
    sent(params.at[0], jnp.where(helps, 1, 0))
    sent(row_out, jnp.where(owns, samp_size * gene_size - 1, 0))


def solution(mesh):
    samp_size, gene_size = mesh.shape["samp"], mesh.shape["gene"]

    def local(
        genotypes, allele_freq, sample_weight, residual, variant_weight, block_gene, gene_variants
    ):
        local_rows, columns = genotypes.shape
        local_blocks = columns // BLK
        fields = sample_weight.shape[0]
        genes = gene_variants.shape[0]
        depth = fields * local_rows // BLK
        width = -(-(STATS * genes + 1) // BLK) * BLK
        owner_low, owner_size = owner_range(samp_size, local_blocks)
        owned = local_blocks // owner_size
        both = pl.pallas_call(
            functools.partial(kernel, samp_size, gene_size, owner_low, owner_size),
            out_shape=pltpu.VMEM((2, genes), jnp.float32),
            in_specs=[pl.BlockSpec(memory_space=pl.ANY)] * 7,
            out_specs=pl.BlockSpec(memory_space=pltpu.VMEM),
            scratch_shapes=[
                pltpu.VMEM((local_rows, columns), jnp.int32),
                pltpu.VMEM((fields, local_rows), jnp.float32),
                pltpu.VMEM((fields, local_rows), jnp.float32),
                pltpu.VMEM((1, block_gene.shape[0]), jnp.int32),
                pltpu.VMEM((1, genes), jnp.int32),
                pltpu.VMEM((PAIR, 2, local_blocks, BLK), jnp.float32),
                pltpu.VMEM((2 * depth, BLK), jnp.float32),
                pltpu.VMEM((samp_size, 2 * depth, BLK), jnp.float32),
                pltpu.VMEM((PAIR, samp_size, local_rows, owned * BLK), jnp.int32),
                pltpu.VMEM((PAIR * owned, depth, BLK, BLK), jnp.float32),
                pltpu.VMEM((PAIR * owned, BLK, BLK), jnp.float32),
                pltpu.VMEM((1, width), jnp.float32),
                pltpu.VMEM((owner_size * gene_size // PAIR, 1, width), jnp.float32),
                pltpu.SemaphoreType.DMA((3,)),
                pltpu.SemaphoreType.DMA,
                pltpu.SemaphoreType.DMA((samp_size // CHUNK,)),
                pltpu.SemaphoreType.DMA((PAIR, samp_size // CHUNK)),
                pltpu.SemaphoreType.DMA,
                pltpu.SemaphoreType.DMA,
            ],
            compiler_params=pltpu.CompilerParams(collective_id=0, has_side_effects=True),
        )(
            genotypes,
            allele_freq.reshape(local_blocks, BLK),
            sample_weight,
            residual,
            variant_weight.reshape(local_blocks, BLK),
            block_gene.reshape(1, -1),
            gene_variants.reshape(1, -1),
        )
        return both[0], both[1]

    placed = (P("samp", "gene"), P("gene"), P(None, "samp"), P(None, "samp"), P("gene"), P(), P())
    return jax.shard_map(local, mesh=mesh, in_specs=placed, out_specs=(P(), P()), check_vma=False)
```

```python
import functools

import jax
import jax.numpy as jnp
from jax import lax
from jax.experimental import pallas as pl
from jax.experimental.pallas import tpu as pltpu
from jax.sharding import PartitionSpec as P

BLK = 128
MESH = pl.DeviceIdType.MESH
STATS = 5
SCORE = 16
PAIR = 2
CHUNK = 2
LEAD_ORDER = ((1, 0), (1, 3), (1, 2), (1, 1), (0, 0), (0, 3), (0, 2), (0, 1))
HELP_ORDER = ((0, 0), (0, 3), (0, 2), (0, 1))


def lane_sum(row):
    return jnp.sum(row, axis=1, keepdims=True)


def owner_range(samp_size, local_blocks):
    low = samp_size // 4
    size = max(1, samp_size // 2)
    while local_blocks % (PAIR * size) and size > 1:
        size -= 1
    return low, size


def flip(samp, step):
    peer, bit = samp, 1
    while bit <= step:
        if step & bit:
            peer = peer + bit * (1 - 2 * lax.rem(lax.div(samp, bit), 2))
        bit *= 2
    return peer


def kernel(
    samp_size,
    gene_size,
    owner_low,
    owner_size,
    genotypes_hbm,
    freq_hbm,
    weight_hbm,
    residual_hbm,
    variant_hbm,
    block_gene_hbm,
    counts_hbm,
    both_ref,
    words_in,
    weight_in,
    residual_in,
    block_gene_in,
    counts_in,
    params,
    tile_out,
    tiles,
    lead_words,
    kept_words,
    given_words,
    centers,
    pair_weight,
    row_out,
    rows,
    load_sem,
    send_sem,
    tile_sem,
    word_sem,
    param_sem,
    row_sem,
    answer_sem,
    known_sem,
):
    samp = lax.axis_index("samp")
    gene = lax.axis_index("gene")
    side = lax.rem(gene, PAIR)
    lead = gene - side + (PAIR - 1)
    fields, local_rows = weight_in.shape
    group = BLK // local_rows
    depth = fields // group
    local_blocks = params.shape[2]
    owned = local_blocks // owner_size
    taken = owned // 2
    owner_high = owner_low + owner_size
    genes = counts_in.shape[1]
    width = row_out.shape[1]
    leads = side == PAIR - 1
    in_range = jnp.logical_and(samp >= owner_low, samp < owner_high)
    owns = jnp.logical_and(leads, in_range)
    helps = jnp.logical_and(jnp.logical_not(leads), in_range)
    place = samp - owner_low
    row_count = rows.shape[0]

    loads = [
        pltpu.make_async_copy(source, target, load_sem.at[number])
        for number, source, target in (
            (0, genotypes_hbm, words_in),
            (1, weight_hbm, weight_in),
            (1, residual_hbm, residual_in),
            (2, freq_hbm, params.at[side, 0]),
            (2, variant_hbm, params.at[side, 1]),
            (2, block_gene_hbm, block_gene_in),
            (2, counts_hbm, counts_in),
        )
    ]
    for load in loads[1:] + loads[:1]:
        load.start()

    def signal(semaphore, samp_to, gene_to):
        pl.semaphore_signal(
            semaphore,
            inc=1,
            device_id={"samp": samp_to, "gene": gene_to},
            device_id_type=MESH,
        )

    barrier = pltpu.get_barrier_semaphore()

    @pl.when(leads)
    def _():
        signal(barrier, samp, gene - 1)

    @pl.when(in_range)
    def _():
        @pl.loop(1, samp_size)
        def _(step):
            samp_to = lax.rem(samp + step, samp_size)
            signal(barrier, samp_to, gene)

            @pl.when(leads)
            def _():
                signal(barrier, samp_to, gene - 1)

    for gene_to in range(PAIR, gene_size):

        @pl.when(gene_to > lead)
        def _(gene_to=gene_to):
            signal(barrier, samp, gene_to)

    loads[1].wait()
    loads[2].wait()
    own_tile = jnp.concatenate(
        [
            jnp.concatenate(
                [part[lanes * depth : (lanes + 1) * depth] for lanes in range(group)], axis=1
            )
            for part in (weight_in[...], residual_in[...])
        ],
        axis=0,
    )
    tile_out[...] = own_tile
    tiles[samp] = own_tile

    targets = jnp.where(in_range, owner_size - 1, owner_size)
    earlier = lead - (PAIR - 1)
    pl.semaphore_wait(barrier, jnp.where(leads, targets, 2 * targets + 1) + earlier)

    chunk = lax.div(samp, CHUNK)

    def tile_copy(owner):
        return pltpu.make_async_remote_copy(
            src_ref=tile_out,
            dst_ref=tiles.at[samp],
            send_sem=send_sem,
            recv_sem=tile_sem.at[chunk],
            device_id={"samp": owner, "gene": gene},
            device_id_type=MESH,
        )

    def word_copy(target, first, count, gene_to):
        def copy(owner):
            start = pl.multiple_of(((owner - owner_low) * owned + first) * BLK, BLK)
            return pltpu.make_async_remote_copy(
                src_ref=words_in.at[:, pl.ds(start, count * BLK)],
                dst_ref=target.at[samp],
                send_sem=send_sem,
                recv_sem=word_sem.at[side, chunk],
                device_id={"samp": owner, "gene": gene_to},
                device_id_type=MESH,
            )

        return copy

    upward = 2 * samp < 2 * owner_low + owner_size

    def to_owner(send, order, here=False):
        owner = jnp.where(upward, owner_high - 1 - order, owner_low + order)
        if here:
            send(owner).start()
        else:

            @pl.when(owner != samp)
            def _():
                send(owner).start()

    def to_owners(send):
        for order in range(owner_size):
            to_owner(send, order)

    to_owners(tile_copy)
    loads[0].wait()

    @pl.when(leads)
    def _():
        to_owners(word_copy(lead_words, 0, owned, gene))

    @pl.when(jnp.logical_not(leads))
    def _():
        for order in range(owner_size):
            to_owner(word_copy(kept_words, taken, owned - taken, gene), order)
            if taken:
                to_owner(word_copy(given_words, 0, taken, lead), order, True)

    for gene_to in range(gene_size - PAIR):

        @pl.when(gene_to < earlier)
        def _(gene_to=gene_to):
            signal(answer_sem, samp, gene_to)

    for load in loads[3:]:
        load.wait()
    later = gene_size - 1 - lead

    @pl.when(jnp.logical_and(helps, taken > 0))
    def _():
        pltpu.make_async_remote_copy(
            src_ref=params.at[0],
            dst_ref=params.at[0],
            send_sem=send_sem,
            recv_sem=param_sem,
            device_id={"samp": samp, "gene": lead},
            device_id_type=MESH,
        ).start()

    @pl.when(later > 0)
    def _():
        pl.semaphore_wait(answer_sem, later)

        @pl.loop(owner_low, owner_high)
        def _(owner):
            @pl.when(owner != samp)
            def _():
                signal(known_sem, owner, gene)

    def own(streams, order):
        block_gene = block_gene_in[...].astype(jnp.float32)
        counts = counts_in[...].astype(jnp.float32)
        block_lane = lax.broadcasted_iota(jnp.int32, block_gene.shape, 1)
        gene_lane = lax.broadcasted_iota(jnp.int32, counts.shape, 1).astype(jnp.float32)
        column = lax.broadcasted_iota(jnp.int32, (1, BLK), 1).astype(jnp.float32)
        stat_sub = lax.broadcasted_iota(jnp.int32, (8, width), 0)
        stat_lane = lax.broadcasted_iota(jnp.int32, (8, width), 1) - stat_sub * genes
        effective, places, numbers = [], [], {}
        for from_side, (buffer, first_block, count) in streams.items():
            for block in range(count):
                number = numbers[from_side, block] = len(numbers)
                local_block = place * owned + first_block + block
                block_id = (lead - (PAIR - 1) + from_side) * local_blocks + local_block
                gene_of = lane_sum(jnp.where(block_lane == block_id, block_gene, 0.0))
                first = lane_sum(jnp.where(block_gene < gene_of, 1.0, 0.0))
                counted = lane_sum(jnp.where(gene_lane == gene_of, counts, 0.0))
                block_float = jnp.zeros((1, 1), jnp.float32) + block_id.astype(jnp.float32)
                live = (block_float - first) * BLK + column < counted
                weights = jnp.where(live, params[from_side, 1, pl.ds(local_block, 1), :], 0.0)
                effective.append(weights)
                across = jnp.broadcast_to(weights, (BLK, BLK))
                pair_weight[number] = across * across.T
                freq = params[from_side, 0, pl.ds(local_block, 1), :]
                center = 2.0 * jnp.broadcast_to(freq, (BLK, BLK)).T
                for level in range(depth):
                    centers[number, level] = center * float(4**level)
                member = stat_lane.astype(jnp.float32) == gene_of
                places.append(jnp.where(member & (stat_sub < STATS), 1.0, 0.0))

        def land(buffer, semaphore):
            pltpu.make_async_copy(buffer, buffer, semaphore).wait()

        def unpack(from_side, peer, power):
            tile = tiles[peer]
            weight, resid = tile[:depth], tile[depth:]
            root = jnp.sqrt(weight)
            score = root * resid
            values = []
            buffer, _, count = streams[from_side]
            for block in range(count):
                part = buffer[peer, :, block * BLK : (block + 1) * BLK]
                turned = jnp.concatenate(
                    [lax.shift_right_logical(part, 2 * depth * lanes) for lanes in range(group)],
                    axis=0,
                ).T
                levels = []
                for level in range(depth):
                    dosage = jnp.bitwise_and(turned, 3 << (2 * level)).astype(jnp.float32)
                    scale = root[level : level + 1] * float(4**-level)
                    center = centers[numbers[from_side, block], level]
                    levels.append(((dosage - center) * scale).astype(jnp.bfloat16))
                values.append(jnp.concatenate(levels, axis=1))
            scores = jnp.concatenate(
                [
                    jnp.broadcast_to(score[level : level + 1], (SCORE, BLK)).astype(jnp.bfloat16)
                    for level in range(depth)
                ],
                axis=1,
            )
            if from_side == main_side:
                power = power + weight * resid * resid
            return (from_side, values, scores), power

        def multiply(unpacked, totals):
            from_side, values, scores = unpacked
            totals = list(totals)
            for block in range(streams[from_side][2]):
                number = numbers[from_side, block]
                totals[number] = totals[number] + lax.dot_general(
                    jnp.concatenate([values[block], scores], axis=0),
                    values[block],
                    (((1,), (1,)), ((), ())),
                    preferred_element_type=jnp.float32,
                )
            return tuple(totals)

        def wait_chunk(from_side, from_chunk, own):
            first = from_chunk * CHUNK
            buffer = streams[from_side][0]
            if from_side != main_side:
                land(buffer.at[pl.ds(first, CHUNK)], word_sem.at[from_side, from_chunk])
            elif own:
                peer = flip(samp, 1)
                land(tiles.at[peer], tile_sem.at[from_chunk])
                land(buffer.at[peer], word_sem.at[from_side, from_chunk])
            else:
                land(tiles.at[pl.ds(first, CHUNK)], tile_sem.at[from_chunk])
                land(buffer.at[pl.ds(first, CHUNK)], word_sem.at[from_side, from_chunk])

        main_side = max(streams)
        buffer, first_block, count = streams[main_side]
        own_start = pl.multiple_of((place * owned + first_block) * BLK, BLK)
        buffer[samp] = words_in[:, pl.ds(own_start, count * BLK)]
        diagonal = lax.broadcasted_iota(jnp.int32, (BLK, BLK), 0) == lax.broadcasted_iota(
            jnp.int32, (BLK, BLK), 1
        )

        def finish(from_side, totals, message):
            for block in range(streams[from_side][2]):
                number = numbers[from_side, block]
                total = totals[number]
                weighted = total[:BLK] * pair_weight[number]
                score = effective[number] * total[BLK : BLK + 1]
                sums = [
                    score,
                    jnp.sum(weighted, axis=0, keepdims=True),
                    score * score,
                    jnp.sum(jnp.where(diagonal, weighted, 0.0), axis=0, keepdims=True),
                    jnp.sum(weighted * weighted, axis=0, keepdims=True),
                    jnp.zeros((8 - STATS, BLK), jnp.float32),
                ]
                message = message + lane_sum(jnp.concatenate(sums, axis=0)) * places[number]
            return message

        chunks = samp_size // CHUNK
        totals = tuple(jnp.zeros((BLK + SCORE, BLK), jnp.float32) for _ in numbers)
        power = jnp.zeros((depth, BLK), jnp.float32)
        message = jnp.zeros((8, width), jnp.float32)
        finished = set()
        if chunks == 4:
            waiting = None
            for place_in_order, (from_side, step) in enumerate(order):
                from_chunk = flip(chunk, step)
                wait_chunk(from_side, from_chunk, step == 0)
                for member in range(CHUNK):
                    ahead, power = unpack(from_side, from_chunk * CHUNK + member, power)
                    if waiting is not None:
                        totals = multiply(waiting, totals)
                    waiting = ahead
                for done in streams:
                    left = [turn for turn in order[place_in_order:] if turn[0] == done]
                    if not left and done not in finished and done != from_side:
                        message = finish(done, totals, message)
                        finished.add(done)
            totals = multiply(waiting, totals)
        else:

            def add_chunk(from_chunk, totals, power, own):
                for from_side in sorted(streams, reverse=True):
                    wait_chunk(from_side, from_chunk, own)
                    for member in range(CHUNK):
                        ahead, power = unpack(from_side, from_chunk * CHUNK + member, power)
                        totals = multiply(ahead, totals)
                return totals, power

            totals, power = lax.fori_loop(
                1,
                chunks,
                lambda step, carry: add_chunk(lax.rem(chunk + step, chunks), *carry, False),
                add_chunk(chunk, totals, power, True),
            )

        for from_side in streams:
            if from_side not in finished:
                message = finish(from_side, totals, message)
        squares = lane_sum(jnp.sum(power, axis=0, keepdims=True))
        lane = lax.broadcasted_iota(jnp.int32, (1, width), 1)
        reports = jnp.logical_and(place == 0, gene == PAIR - 1).astype(jnp.float32)
        row = jnp.sum(message, axis=0, keepdims=True) + jnp.where(
            lane == STATS * genes, squares * reports, 0.0
        )
        @pl.when(later > 0)
        def _():
            pl.semaphore_wait(known_sem, samp_size - 1)

        row_out[...] = row
        slot = place * gene_size + gene
        rows[slot] = row

        @pl.loop(0, samp_size)
        def _(samp_to):
            for gene_to in range(gene_size):

                @pl.when(jnp.logical_or(samp_to != samp, gene_to != gene))
                def _(gene_to=gene_to):
                    pltpu.make_async_remote_copy(
                        src_ref=row_out,
                        dst_ref=rows.at[slot],
                        send_sem=send_sem,
                        recv_sem=row_sem,
                        device_id={"samp": samp_to, "gene": gene_to},
                        device_id_type=MESH,
                    ).start()

    lead_streams = {PAIR - 1: (lead_words, 0, owned)}
    if taken:
        lead_streams[0] = (given_words, 0, taken)

    @pl.when(owns)
    def _():
        if taken:
            landed = params.at[0]
            pltpu.make_async_copy(landed, landed, param_sem).wait()
        own(lead_streams, [turn for turn in LEAD_ORDER if turn[0] in lead_streams])

    @pl.when(helps)
    def _():
        own({0: (kept_words, taken, owned - taken)}, HELP_ORDER)

    @pl.when(in_range)
    def _():
        landed = rows.at[pl.ds(0, row_count - 1)]
        pltpu.make_async_copy(landed, landed, row_sem).wait()

    @pl.when(jnp.logical_not(in_range))
    def _():
        pltpu.make_async_copy(rows, rows, row_sem).wait()

    totals = jnp.sum(rows[...], axis=0)
    parts = [totals[:, stat * genes : (stat + 1) * genes] for stat in range(STATS)]
    variance = totals[:, STATS * genes : STATS * genes + 1] / (fields * local_rows * samp_size)
    both_ref[0:1] = parts[0] / jnp.sqrt(variance * parts[1])
    both_ref[1:2] = (parts[2] - variance * parts[3]) / (
        variance * jnp.sqrt(2.0 * parts[4])
    )

    def sent(buffer, count):
        @pl.loop(0, count)
        def _(_):
            pltpu.make_async_copy(buffer, buffer, send_sem).wait()

    sent(tile_out, targets)
    sent(lead_words.at[0], jnp.where(leads, targets, 0))
    sent(kept_words.at[0], jnp.where(leads, 0, targets))
    if taken:
        sent(given_words.at[0], jnp.where(leads, 0, owner_size))
        sent(params.at[0], jnp.where(helps, 1, 0))
    sent(row_out, jnp.where(in_range, samp_size * gene_size - 1, 0))


def solution(mesh):
    samp_size, gene_size = mesh.shape["samp"], mesh.shape["gene"]

    def local(
        genotypes, allele_freq, sample_weight, residual, variant_weight, block_gene, gene_variants
    ):
        local_rows, columns = genotypes.shape
        local_blocks = columns // BLK
        fields = sample_weight.shape[0]
        genes = gene_variants.shape[0]
        depth = fields * local_rows // BLK
        width = -(-(STATS * genes + 1) // BLK) * BLK
        owner_low, owner_size = owner_range(samp_size, local_blocks)
        owned = local_blocks // owner_size
        taken = owned // 2
        both = pl.pallas_call(
            functools.partial(kernel, samp_size, gene_size, owner_low, owner_size),
            out_shape=pltpu.VMEM((2, genes), jnp.float32),
            in_specs=[pl.BlockSpec(memory_space=pl.ANY)] * 7,
            out_specs=pl.BlockSpec(memory_space=pltpu.VMEM),
            scratch_shapes=[
                pltpu.VMEM((local_rows, columns), jnp.int32),
                pltpu.VMEM((fields, local_rows), jnp.float32),
                pltpu.VMEM((fields, local_rows), jnp.float32),
                pltpu.VMEM((1, block_gene.shape[0]), jnp.int32),
                pltpu.VMEM((1, genes), jnp.int32),
                pltpu.VMEM((PAIR, 2, local_blocks, BLK), jnp.float32),
                pltpu.VMEM((2 * depth, BLK), jnp.float32),
                pltpu.VMEM((samp_size, 2 * depth, BLK), jnp.float32),
                pltpu.VMEM((samp_size, local_rows, owned * BLK), jnp.int32),
                pltpu.VMEM((samp_size, local_rows, (owned - taken) * BLK), jnp.int32),
                pltpu.VMEM((samp_size, local_rows, max(taken, 1) * BLK), jnp.int32),
                pltpu.VMEM((owned + taken, depth, BLK, BLK), jnp.float32),
                pltpu.VMEM((owned + taken, BLK, BLK), jnp.float32),
                pltpu.VMEM((1, width), jnp.float32),
                pltpu.VMEM((owner_size * gene_size, 1, width), jnp.float32),
                pltpu.SemaphoreType.DMA((3,)),
                pltpu.SemaphoreType.DMA,
                pltpu.SemaphoreType.DMA((samp_size // CHUNK,)),
                pltpu.SemaphoreType.DMA((PAIR, samp_size // CHUNK)),
                pltpu.SemaphoreType.DMA,
                pltpu.SemaphoreType.DMA,
                pltpu.SemaphoreType.REGULAR,
                pltpu.SemaphoreType.REGULAR,
            ],
            compiler_params=pltpu.CompilerParams(collective_id=0, has_side_effects=True),
        )(
            genotypes,
            allele_freq.reshape(local_blocks, BLK),
            sample_weight,
            residual,
            variant_weight.reshape(local_blocks, BLK),
            block_gene.reshape(1, -1),
            gene_variants.reshape(1, -1),
        )
        return both[0], both[1]

    placed = (P("samp", "gene"), P("gene"), P(None, "samp"), P(None, "samp"), P("gene"), P(), P())
    return jax.shard_map(local, mesh=mesh, in_specs=placed, out_specs=(P(), P()), check_vma=False)
```

```python
import functools

import jax
import jax.numpy as jnp
from jax import lax
from jax.experimental import pallas as pl
from jax.experimental.pallas import tpu as pltpu
from jax.sharding import PartitionSpec as P

BLK = 128
MESH = pl.DeviceIdType.MESH
STATS = 5
SCORE = 16
PAIR = 2
TURNS = (
    (1, (1,)),
    (0, (0, 1)),
    (1, (6, 7)),
    (1, (4, 5)),
    (0, (4, 5)),
    (1, (2, 3)),
    (0, (6, 7)),
    (0, (2, 3)),
)


def lane_sum(row):
    return jnp.sum(row, axis=1, keepdims=True)


def owner_range(samp_size, local_blocks):
    low = samp_size // 4
    size = max(1, samp_size // 2)
    while local_blocks % size:
        size -= 1
    return low, size


def flip(samp, step):
    peer, bit = samp, 1
    while bit <= step:
        if step & bit:
            peer = peer + bit * (1 - 2 * lax.rem(lax.div(samp, bit), 2))
        bit *= 2
    return peer


def kernel(
    samp_size,
    gene_size,
    owner_low,
    owner_size,
    genotypes_hbm,
    freq_hbm,
    weight_hbm,
    residual_hbm,
    variant_hbm,
    block_gene_hbm,
    counts_hbm,
    both_ref,
    words_in,
    weight_in,
    residual_in,
    block_gene_in,
    counts_in,
    params,
    tile_out,
    tiles,
    lead_words,
    given_words,
    centers,
    pair_weight,
    row_out,
    rows,
    load_sem,
    send_sem,
    tile_sem,
    lead_sem,
    given_sem,
    param_sem,
    row_sem,
    answer_sem,
    known_sem,
):
    samp = lax.axis_index("samp")
    gene = lax.axis_index("gene")
    side = lax.rem(gene, PAIR)
    lead = gene - side + (PAIR - 1)
    fields, local_rows = weight_in.shape
    group = BLK // local_rows
    depth = fields // group
    local_blocks = params.shape[2]
    owned = local_blocks // owner_size
    owner_high = owner_low + owner_size
    genes = counts_in.shape[1]
    width = row_out.shape[1]
    leads = side == PAIR - 1
    in_range = jnp.logical_and(samp >= owner_low, samp < owner_high)
    owns = jnp.logical_and(leads, in_range)
    helps = jnp.logical_and(jnp.logical_not(leads), in_range)
    place = samp - owner_low
    row_count = rows.shape[0]

    loads = [
        pltpu.make_async_copy(source, target, load_sem.at[number])
        for number, source, target in (
            (0, genotypes_hbm, words_in),
            (1, weight_hbm, weight_in),
            (1, residual_hbm, residual_in),
            (2, freq_hbm, params.at[side, 0]),
            (2, variant_hbm, params.at[side, 1]),
            (2, block_gene_hbm, block_gene_in),
            (2, counts_hbm, counts_in),
        )
    ]
    for load in loads[1:] + loads[:1]:
        load.start()

    def signal(semaphore, samp_to, gene_to):
        pl.semaphore_signal(
            semaphore,
            inc=1,
            device_id={"samp": samp_to, "gene": gene_to},
            device_id_type=MESH,
        )

    barrier = pltpu.get_barrier_semaphore()

    @pl.when(leads)
    def _():
        signal(barrier, samp, gene - 1)

    @pl.when(owns)
    def _():
        @pl.loop(1, samp_size)
        def _(step):
            for other in range(PAIR):
                signal(barrier, lax.rem(samp + step, samp_size), gene - other)

    for gene_to in range(PAIR, gene_size):

        @pl.when(gene_to > lead)
        def _(gene_to=gene_to):
            signal(barrier, samp, gene_to)

    loads[1].wait()
    loads[2].wait()
    own_tile = jnp.concatenate(
        [
            jnp.concatenate(
                [part[lanes * depth : (lanes + 1) * depth] for lanes in range(group)], axis=1
            )
            for part in (weight_in[...], residual_in[...])
        ],
        axis=0,
    )
    tile_out[...] = own_tile
    tiles[samp] = own_tile

    targets = jnp.where(in_range, owner_size - 1, owner_size)
    earlier = lead - (PAIR - 1)
    pl.semaphore_wait(barrier, jnp.where(leads, targets, targets + 1) + earlier)

    def tile_copy(owner):
        return pltpu.make_async_remote_copy(
            src_ref=tile_out,
            dst_ref=tiles.at[samp],
            send_sem=send_sem,
            recv_sem=tile_sem.at[lax.div(samp, 2)],
            device_id={"samp": owner, "gene": gene},
            device_id_type=MESH,
        )

    def word_copy(target, semaphore):
        def copy(owner):
            start = pl.multiple_of((owner - owner_low) * (owned * BLK), BLK)
            return pltpu.make_async_remote_copy(
                src_ref=words_in.at[:, pl.ds(start, owned * BLK)],
                dst_ref=target.at[samp],
                send_sem=send_sem,
                recv_sem=semaphore,
                device_id={"samp": owner, "gene": lead},
                device_id_type=MESH,
            )

        return copy

    upward = 2 * samp < 2 * owner_low + owner_size

    def to_owner(send, order, here=False):
        owner = jnp.where(upward, owner_high - 1 - order, owner_low + order)
        if here:
            send(owner).start()
        else:

            @pl.when(owner != samp)
            def _():
                send(owner).start()

    def to_owners(send, here=False):
        for order in range(owner_size):
            to_owner(send, order, here)

    @pl.when(leads)
    def _():
        to_owners(tile_copy)

    loads[0].wait()

    @pl.when(leads)
    def _():
        to_owners(word_copy(lead_words, lead_sem.at[lax.div(samp, 2)]))

    @pl.when(jnp.logical_not(leads))
    def _():
        to_owners(word_copy(given_words, given_sem.at[lax.div(samp, 2)]), True)

    for gene_to in range(gene_size - PAIR):

        @pl.when(gene_to < earlier)
        def _(gene_to=gene_to):
            signal(answer_sem, samp, gene_to)

    for load in loads[3:]:
        load.wait()
    later = gene_size - 1 - lead

    @pl.when(helps)
    def _():
        pltpu.make_async_remote_copy(
            src_ref=params.at[0],
            dst_ref=params.at[0],
            send_sem=send_sem,
            recv_sem=param_sem,
            device_id={"samp": samp, "gene": lead},
            device_id_type=MESH,
        ).start()

    @pl.when(later > 0)
    def _():
        pl.semaphore_wait(answer_sem, later)

        @pl.loop(owner_low, owner_high)
        def _(owner):
            @pl.when(jnp.logical_and(owner != samp, leads))
            def _():
                signal(known_sem, owner, gene)

    @pl.when(owns)
    def _():
        pltpu.make_async_copy(params.at[0], params.at[0], param_sem).wait()
        block_gene = block_gene_in[...].astype(jnp.float32)
        counts = counts_in[...].astype(jnp.float32)
        block_lane = lax.broadcasted_iota(jnp.int32, block_gene.shape, 1)
        gene_lane = lax.broadcasted_iota(jnp.int32, counts.shape, 1).astype(jnp.float32)
        column = lax.broadcasted_iota(jnp.int32, (1, BLK), 1).astype(jnp.float32)
        stat_sub = lax.broadcasted_iota(jnp.int32, (8, width), 0)
        stat_lane = lax.broadcasted_iota(jnp.int32, (8, width), 1) - stat_sub * genes
        effective, places = [], []
        for number in range(PAIR * owned):
            from_side, block = divmod(number, owned)
            local_block = place * owned + block
            block_id = (lead - (PAIR - 1) + from_side) * local_blocks + local_block
            gene_of = lane_sum(jnp.where(block_lane == block_id, block_gene, 0.0))
            first = lane_sum(jnp.where(block_gene < gene_of, 1.0, 0.0))
            counted = lane_sum(jnp.where(gene_lane == gene_of, counts, 0.0))
            block_float = jnp.zeros((1, 1), jnp.float32) + block_id.astype(jnp.float32)
            live = (block_float - first) * BLK + column < counted
            weights = jnp.where(live, params[from_side, 1, pl.ds(local_block, 1), :], 0.0)
            effective.append(weights)
            across = jnp.broadcast_to(weights, (BLK, BLK))
            pair_weight[number] = across * across.T
            freq = params[from_side, 0, pl.ds(local_block, 1), :]
            center = 2.0 * jnp.broadcast_to(freq, (BLK, BLK)).T
            for level in range(depth):
                centers[number, level] = center * float(4**level)
            member = stat_lane.astype(jnp.float32) == gene_of
            places.append(jnp.where(member & (stat_sub < STATS), 1.0, 0.0))

        def land(buffer, semaphore):
            pltpu.make_async_copy(buffer, buffer, semaphore).wait()

        def unpack(from_side, peer, power):
            tile = tiles[peer]
            weight, resid = tile[:depth], tile[depth:]
            root = jnp.sqrt(weight)
            score = root * resid
            if from_side:
                power = power + weight * resid * resid
            values = []
            buffer = lead_words if from_side else given_words
            for block in range(owned):
                part = buffer[peer, :, block * BLK : (block + 1) * BLK]
                turned = jnp.concatenate(
                    [lax.shift_right_logical(part, 2 * depth * lanes) for lanes in range(group)],
                    axis=0,
                ).T
                levels = []
                for level in range(depth):
                    dosage = jnp.bitwise_and(turned, 3 << (2 * level)).astype(jnp.float32)
                    scale = root[level : level + 1] * float(4**-level)
                    center = centers[from_side * owned + block, level]
                    levels.append(((dosage - center) * scale).astype(jnp.bfloat16))
                values.append(jnp.concatenate(levels, axis=1))
            scores = jnp.concatenate(
                [
                    jnp.broadcast_to(score[level : level + 1], (SCORE, BLK)).astype(jnp.bfloat16)
                    for level in range(depth)
                ],
                axis=1,
            )
            return (from_side, values, scores), power

        def multiply(unpacked, totals):
            from_side, values, scores = unpacked
            totals = list(totals)
            for block in range(owned):
                number = from_side * owned + block
                totals[number] = totals[number] + lax.dot_general(
                    jnp.concatenate([values[block], scores], axis=0),
                    values[block],
                    (((1,), (1,)), ((), ())),
                    preferred_element_type=jnp.float32,
                )
            return tuple(totals)

        own_start = pl.multiple_of(place * (owned * BLK), BLK)
        lead_words[samp] = words_in[:, pl.ds(own_start, owned * BLK)]

        diagonal = lax.broadcasted_iota(jnp.int32, (BLK, BLK), 0) == lax.broadcasted_iota(
            jnp.int32, (BLK, BLK), 1
        )

        def finish(from_side, totals, message):
            for block in range(owned):
                number = from_side * owned + block
                total = totals[number]
                weighted = total[:BLK] * pair_weight[number]
                score = effective[number] * total[BLK : BLK + 1]
                sums = [
                    score,
                    jnp.sum(weighted, axis=0, keepdims=True),
                    score * score,
                    jnp.sum(jnp.where(diagonal, weighted, 0.0), axis=0, keepdims=True),
                    jnp.sum(weighted * weighted, axis=0, keepdims=True),
                    jnp.zeros((8 - STATS, BLK), jnp.float32),
                ]
                message = message + lane_sum(jnp.concatenate(sums, axis=0)) * places[number]
            return message

        def land_lead(first, count):
            two = lax.div(first, 2)
            land(tiles.at[pl.ds(first, count)], tile_sem.at[two])
            land(lead_words.at[pl.ds(first, count)], lead_sem.at[two])

        def land_given(first):
            land(given_words.at[pl.ds(first, 2)], given_sem.at[lax.div(first, 2)])

        message = jnp.zeros((8, width), jnp.float32)
        power = jnp.zeros((depth, BLK), jnp.float32)
        totals = tuple(jnp.zeros((BLK + SCORE, BLK), jnp.float32) for _ in range(PAIR * owned))
        if samp_size == 8:
            waiting, power = unpack(PAIR - 1, samp, power)
            for number, (from_side, steps) in enumerate(TURNS):
                peers = [flip(samp, step) for step in steps]
                pair = samp - lax.rem(samp, 2)
                if steps[0] > 1:
                    pair = flip(pair, steps[0])
                if from_side == 0:
                    land_given(pair)
                elif len(steps) == 1:
                    land_lead(peers[0], 1)
                else:
                    land_lead(pair, 2)
                for peer in peers:
                    ahead, power = unpack(from_side, peer, power)
                    totals = multiply(waiting, totals)
                    waiting = ahead
                if all(side == 0 for side, _ in TURNS[number:]) and TURNS[number - 1][0]:
                    message = finish(PAIR - 1, totals, message)
            totals = multiply(waiting, totals)
            message = finish(0, totals, message)
        else:
            ahead, power = unpack(PAIR - 1, samp, power)
            totals = multiply(ahead, totals)
            partner = samp + 1 - 2 * lax.rem(samp, 2)
            land_lead(partner, 1)
            ahead, power = unpack(PAIR - 1, partner, power)
            totals = multiply(ahead, totals)

            def add_lead(step, carry):
                totals, power = carry
                first = 2 * lax.rem(lax.div(samp, 2) + step, samp_size // 2)
                land_lead(first, 2)
                for member in range(2):
                    ahead, power = unpack(PAIR - 1, first + member, power)
                    totals = multiply(ahead, totals)
                return totals, power

            def add_given(two, totals):
                land_given(two * 2)
                for member in range(2):
                    totals = multiply(unpack(0, two * 2 + member, power)[0], totals)
                return totals

            totals, power = lax.fori_loop(1, samp_size // 2, add_lead, (totals, power))
            totals = lax.fori_loop(0, samp_size // 2, add_given, totals)
            for from_side in range(PAIR):
                message = finish(from_side, totals, message)
        squares = lane_sum(jnp.sum(power, axis=0, keepdims=True))
        reports = jnp.logical_and(place == 0, gene == PAIR - 1).astype(jnp.float32)
        lane = lax.broadcasted_iota(jnp.int32, (8, width), 1)
        message = message + jnp.where(
            (lane == STATS * genes) & (stat_sub == 0), squares * reports, 0.0
        )
        row = jnp.sum(message, axis=0, keepdims=True)

        @pl.when(later > 0)
        def _():
            pl.semaphore_wait(known_sem, samp_size - 1)

        row_out[...] = row
        slot = place * (gene_size // PAIR) + lax.div(gene, PAIR)
        rows[slot] = row

        @pl.loop(0, samp_size)
        def _(samp_to):
            for gene_to in range(gene_size):

                @pl.when(jnp.logical_or(samp_to != samp, gene_to != gene))
                def _(gene_to=gene_to):
                    pltpu.make_async_remote_copy(
                        src_ref=row_out,
                        dst_ref=rows.at[slot],
                        send_sem=send_sem,
                        recv_sem=row_sem,
                        device_id={"samp": samp_to, "gene": gene_to},
                        device_id_type=MESH,
                    ).start()

    @pl.when(owns)
    def _():
        landed = rows.at[pl.ds(0, row_count - 1)]
        pltpu.make_async_copy(landed, landed, row_sem).wait()

    @pl.when(jnp.logical_not(owns))
    def _():
        pltpu.make_async_copy(rows, rows, row_sem).wait()

    totals = jnp.sum(rows[...], axis=0)
    parts = [totals[:, stat * genes : (stat + 1) * genes] for stat in range(STATS)]
    variance = totals[:, STATS * genes : STATS * genes + 1] / (fields * local_rows * samp_size)
    both_ref[0:1] = parts[0] / jnp.sqrt(variance * parts[1])
    both_ref[1:2] = (parts[2] - variance * parts[3]) / (
        variance * jnp.sqrt(2.0 * parts[4])
    )

    def sent(buffer, count):
        @pl.loop(0, count)
        def _(_):
            pltpu.make_async_copy(buffer, buffer, send_sem).wait()

    sent(tile_out, jnp.where(leads, targets, 0))
    sent(lead_words.at[0], jnp.where(leads, targets, owner_size))
    sent(params.at[0], jnp.where(helps, 1, 0))
    sent(row_out, jnp.where(owns, samp_size * gene_size - 1, 0))


def solution(mesh):
    samp_size, gene_size = mesh.shape["samp"], mesh.shape["gene"]

    def local(
        genotypes, allele_freq, sample_weight, residual, variant_weight, block_gene, gene_variants
    ):
        local_rows, columns = genotypes.shape
        local_blocks = columns // BLK
        fields = sample_weight.shape[0]
        genes = gene_variants.shape[0]
        depth = fields * local_rows // BLK
        width = -(-(STATS * genes + 1) // BLK) * BLK
        owner_low, owner_size = owner_range(samp_size, local_blocks)
        owned = local_blocks // owner_size
        both = pl.pallas_call(
            functools.partial(kernel, samp_size, gene_size, owner_low, owner_size),
            out_shape=pltpu.VMEM((2, genes), jnp.float32),
            in_specs=[pl.BlockSpec(memory_space=pl.ANY)] * 7,
            out_specs=pl.BlockSpec(memory_space=pltpu.VMEM),
            scratch_shapes=[
                pltpu.VMEM((local_rows, columns), jnp.int32),
                pltpu.VMEM((fields, local_rows), jnp.float32),
                pltpu.VMEM((fields, local_rows), jnp.float32),
                pltpu.VMEM((1, block_gene.shape[0]), jnp.int32),
                pltpu.VMEM((1, genes), jnp.int32),
                pltpu.VMEM((PAIR, 2, local_blocks, BLK), jnp.float32),
                pltpu.VMEM((2 * depth, BLK), jnp.float32),
                pltpu.VMEM((samp_size, 2 * depth, BLK), jnp.float32),
                pltpu.VMEM((samp_size, local_rows, owned * BLK), jnp.int32),
                pltpu.VMEM((samp_size, local_rows, owned * BLK), jnp.int32),
                pltpu.VMEM((PAIR * owned, depth, BLK, BLK), jnp.float32),
                pltpu.VMEM((PAIR * owned, BLK, BLK), jnp.float32),
                pltpu.VMEM((1, width), jnp.float32),
                pltpu.VMEM((owner_size * gene_size // PAIR, 1, width), jnp.float32),
                pltpu.SemaphoreType.DMA((3,)),
                pltpu.SemaphoreType.DMA,
                pltpu.SemaphoreType.DMA((samp_size // 2,)),
                pltpu.SemaphoreType.DMA((samp_size // 2,)),
                pltpu.SemaphoreType.DMA((samp_size // 2,)),
                pltpu.SemaphoreType.DMA,
                pltpu.SemaphoreType.DMA,
                pltpu.SemaphoreType.REGULAR,
                pltpu.SemaphoreType.REGULAR,
            ],
            compiler_params=pltpu.CompilerParams(collective_id=0, has_side_effects=True),
        )(
            genotypes,
            allele_freq.reshape(local_blocks, BLK),
            sample_weight,
            residual,
            variant_weight.reshape(local_blocks, BLK),
            block_gene.reshape(1, -1),
            gene_variants.reshape(1, -1),
        )
        return both[0], both[1]

    placed = (P("samp", "gene"), P("gene"), P(None, "samp"), P(None, "samp"), P("gene"), P(), P())
    return jax.shard_map(local, mesh=mesh, in_specs=placed, out_specs=(P(), P()), check_vma=False)
```

```python
import functools

import jax
import jax.numpy as jnp
from jax import lax
from jax.experimental import pallas as pl
from jax.experimental.pallas import tpu as pltpu
from jax.sharding import PartitionSpec as P

BLK = 128
MESH = pl.DeviceIdType.MESH
STATS = 5
SCORE = 16
PAIR = 2
TURNS = (
    (1, (1,)),
    (0, (0, 1)),
    (1, (6, 7)),
    (1, (4, 5)),
    (0, (4, 5)),
    (1, (2, 3)),
    (0, (6, 7)),
    (0, (2, 3)),
)


def lane_sum(row):
    return jnp.sum(row, axis=1, keepdims=True)


def owner_range(samp_size, local_blocks):
    low = samp_size // 4
    size = max(1, samp_size // 2)
    while local_blocks % size:
        size -= 1
    return low, size


def flip(samp, step):
    peer, bit = samp, 1
    while bit <= step:
        if step & bit:
            peer = peer + bit * (1 - 2 * lax.rem(lax.div(samp, bit), 2))
        bit *= 2
    return peer


def kernel(
    samp_size,
    gene_size,
    owner_low,
    owner_size,
    genotypes_hbm,
    freq_hbm,
    weight_hbm,
    residual_hbm,
    variant_hbm,
    block_gene_hbm,
    counts_hbm,
    both_ref,
    words_in,
    weight_in,
    residual_in,
    block_gene_in,
    counts_in,
    params,
    tile_out,
    tiles,
    lead_words,
    given_words,
    centers,
    pair_weight,
    row_out,
    rows,
    load_sem,
    send_sem,
    tile_sem,
    lead_sem,
    given_sem,
    param_sem,
    row_sem,
    answer_sem,
    known_sem,
):
    samp = lax.axis_index("samp")
    gene = lax.axis_index("gene")
    side = lax.rem(gene, PAIR)
    lead = gene - side + (PAIR - 1)
    fields, local_rows = weight_in.shape
    group = BLK // local_rows
    depth = fields // group
    local_blocks = params.shape[2]
    owned = local_blocks // owner_size
    owner_high = owner_low + owner_size
    genes = counts_in.shape[1]
    width = row_out.shape[1]
    leads = side == PAIR - 1
    in_range = jnp.logical_and(samp >= owner_low, samp < owner_high)
    owns = jnp.logical_and(leads, in_range)
    helps = jnp.logical_and(jnp.logical_not(leads), in_range)
    place = samp - owner_low
    row_count = rows.shape[0]

    loads = [
        pltpu.make_async_copy(source, target, load_sem.at[number])
        for number, source, target in (
            (0, genotypes_hbm, words_in),
            (1, weight_hbm, weight_in),
            (1, residual_hbm, residual_in),
            (1, freq_hbm, params.at[side, 0]),
            (1, variant_hbm, params.at[side, 1]),
            (1, block_gene_hbm, block_gene_in),
            (1, counts_hbm, counts_in),
        )
    ]
    for load in loads:
        load.start()

    def signal(semaphore, samp_to, gene_to):
        pl.semaphore_signal(
            semaphore,
            inc=1,
            device_id={"samp": samp_to, "gene": gene_to},
            device_id_type=MESH,
        )

    barrier = pltpu.get_barrier_semaphore()

    @pl.when(leads)
    def _():
        signal(barrier, samp, gene - 1)

    @pl.when(owns)
    def _():
        @pl.loop(1, samp_size)
        def _(step):
            for other in range(PAIR):
                signal(barrier, lax.rem(samp + step, samp_size), gene - other)

    for gene_to in range(PAIR, gene_size):

        @pl.when(gene_to > lead)
        def _(gene_to=gene_to):
            signal(barrier, samp, gene_to)

    for load in loads[1:]:
        load.wait()
    own_tile = jnp.concatenate(
        [
            jnp.concatenate(
                [part[lanes * depth : (lanes + 1) * depth] for lanes in range(group)], axis=1
            )
            for part in (weight_in[...], residual_in[...])
        ],
        axis=0,
    )
    tile_out[...] = own_tile
    tiles[samp] = own_tile

    targets = jnp.where(in_range, owner_size - 1, owner_size)
    earlier = lead - (PAIR - 1)
    pl.semaphore_wait(barrier, jnp.where(leads, targets, targets + 1) + earlier)

    def tile_copy(owner):
        return pltpu.make_async_remote_copy(
            src_ref=tile_out,
            dst_ref=tiles.at[samp],
            send_sem=send_sem,
            recv_sem=tile_sem.at[lax.div(samp, 2)],
            device_id={"samp": owner, "gene": gene},
            device_id_type=MESH,
        )

    def word_copy(target, semaphore):
        def copy(owner):
            start = pl.multiple_of((owner - owner_low) * (owned * BLK), BLK)
            return pltpu.make_async_remote_copy(
                src_ref=words_in.at[:, pl.ds(start, owned * BLK)],
                dst_ref=target.at[samp],
                send_sem=send_sem,
                recv_sem=semaphore,
                device_id={"samp": owner, "gene": lead},
                device_id_type=MESH,
            )

        return copy

    upward = 2 * samp < 2 * owner_low + owner_size

    def to_owner(send, order, here=False):
        owner = jnp.where(upward, owner_high - 1 - order, owner_low + order)
        if here:
            send(owner).start()
        else:

            @pl.when(owner != samp)
            def _():
                send(owner).start()

    def to_owners(send, here=False):
        for order in range(owner_size):
            to_owner(send, order, here)

    @pl.when(leads)
    def _():
        to_owners(tile_copy)

    loads[0].wait()

    @pl.when(leads)
    def _():
        to_owners(word_copy(lead_words, lead_sem.at[lax.div(samp, 2)]))

    @pl.when(jnp.logical_not(leads))
    def _():
        to_owners(word_copy(given_words, given_sem.at[lax.div(samp, 2)]), True)

    for gene_to in range(gene_size - PAIR):

        @pl.when(gene_to < earlier)
        def _(gene_to=gene_to):
            signal(answer_sem, samp, gene_to)

    later = gene_size - 1 - lead

    @pl.when(helps)
    def _():
        pltpu.make_async_remote_copy(
            src_ref=params.at[0],
            dst_ref=params.at[0],
            send_sem=send_sem,
            recv_sem=param_sem,
            device_id={"samp": samp, "gene": lead},
            device_id_type=MESH,
        ).start()

    @pl.when(later > 0)
    def _():
        pl.semaphore_wait(answer_sem, later)

        @pl.loop(owner_low, owner_high)
        def _(owner):
            @pl.when(jnp.logical_and(owner != samp, leads))
            def _():
                signal(known_sem, owner, gene)

    @pl.when(owns)
    def _():
        pltpu.make_async_copy(params.at[0], params.at[0], param_sem).wait()
        block_gene = block_gene_in[...].astype(jnp.float32)
        counts = counts_in[...].astype(jnp.float32)
        block_lane = lax.broadcasted_iota(jnp.int32, block_gene.shape, 1)
        gene_lane = lax.broadcasted_iota(jnp.int32, counts.shape, 1).astype(jnp.float32)
        column = lax.broadcasted_iota(jnp.int32, (1, BLK), 1).astype(jnp.float32)
        stat_sub = lax.broadcasted_iota(jnp.int32, (8, width), 0)
        stat_lane = lax.broadcasted_iota(jnp.int32, (8, width), 1) - stat_sub * genes
        effective, places = [], []
        for number in range(PAIR * owned):
            from_side, block = divmod(number, owned)
            local_block = place * owned + block
            block_id = (lead - (PAIR - 1) + from_side) * local_blocks + local_block
            gene_of = lane_sum(jnp.where(block_lane == block_id, block_gene, 0.0))
            first = lane_sum(jnp.where(block_gene < gene_of, 1.0, 0.0))
            counted = lane_sum(jnp.where(gene_lane == gene_of, counts, 0.0))
            block_float = jnp.zeros((1, 1), jnp.float32) + block_id.astype(jnp.float32)
            live = (block_float - first) * BLK + column < counted
            weights = jnp.where(live, params[from_side, 1, pl.ds(local_block, 1), :], 0.0)
            effective.append(weights)
            across = jnp.broadcast_to(weights, (BLK, BLK))
            pair_weight[number] = across * across.T
            freq = params[from_side, 0, pl.ds(local_block, 1), :]
            center = 2.0 * jnp.broadcast_to(freq, (BLK, BLK)).T
            for level in range(depth):
                centers[number, level] = center * float(4**level)
            member = stat_lane.astype(jnp.float32) == gene_of
            places.append(jnp.where(member & (stat_sub < STATS), 1.0, 0.0))

        def land(buffer, semaphore):
            pltpu.make_async_copy(buffer, buffer, semaphore).wait()

        def unpack(from_side, peer, power):
            tile = tiles[peer]
            weight, resid = tile[:depth], tile[depth:]
            root = jnp.sqrt(weight)
            score = root * resid
            if from_side:
                power = power + weight * resid * resid
            values = []
            buffer = lead_words if from_side else given_words
            for block in range(owned):
                part = buffer[peer, :, block * BLK : (block + 1) * BLK]
                turned = jnp.concatenate(
                    [lax.shift_right_logical(part, 2 * depth * lanes) for lanes in range(group)],
                    axis=0,
                ).T
                levels = []
                for level in range(depth):
                    dosage = jnp.bitwise_and(turned, 3 << (2 * level)).astype(jnp.float32)
                    scale = root[level : level + 1] * float(4**-level)
                    center = centers[from_side * owned + block, level]
                    levels.append(((dosage - center) * scale).astype(jnp.bfloat16))
                values.append(jnp.concatenate(levels, axis=1))
            scores = jnp.concatenate(
                [
                    jnp.broadcast_to(score[level : level + 1], (SCORE, BLK)).astype(jnp.bfloat16)
                    for level in range(depth)
                ],
                axis=1,
            )
            return (from_side, values, scores), power

        def multiply(unpacked, totals):
            from_side, values, scores = unpacked
            totals = list(totals)
            for block in range(owned):
                number = from_side * owned + block
                totals[number] = totals[number] + lax.dot_general(
                    jnp.concatenate([values[block], scores], axis=0),
                    values[block],
                    (((1,), (1,)), ((), ())),
                    preferred_element_type=jnp.float32,
                )
            return tuple(totals)

        own_start = pl.multiple_of(place * (owned * BLK), BLK)
        lead_words[samp] = words_in[:, pl.ds(own_start, owned * BLK)]

        diagonal = lax.broadcasted_iota(jnp.int32, (BLK, BLK), 0) == lax.broadcasted_iota(
            jnp.int32, (BLK, BLK), 1
        )

        def finish(from_side, totals, message):
            for block in range(owned):
                number = from_side * owned + block
                total = totals[number]
                weighted = total[:BLK] * pair_weight[number]
                score = effective[number] * total[BLK : BLK + 1]
                sums = [
                    score,
                    jnp.sum(weighted, axis=0, keepdims=True),
                    score * score,
                    jnp.sum(jnp.where(diagonal, weighted, 0.0), axis=0, keepdims=True),
                    jnp.sum(weighted * weighted, axis=0, keepdims=True),
                    jnp.zeros((8 - STATS, BLK), jnp.float32),
                ]
                message = message + lane_sum(jnp.concatenate(sums, axis=0)) * places[number]
            return message

        def land_lead(first, count):
            two = lax.div(first, 2)
            land(tiles.at[pl.ds(first, count)], tile_sem.at[two])
            land(lead_words.at[pl.ds(first, count)], lead_sem.at[two])

        def land_given(first):
            land(given_words.at[pl.ds(first, 2)], given_sem.at[lax.div(first, 2)])

        message = jnp.zeros((8, width), jnp.float32)
        power = jnp.zeros((depth, BLK), jnp.float32)
        totals = tuple(jnp.zeros((BLK + SCORE, BLK), jnp.float32) for _ in range(PAIR * owned))
        if samp_size == 8:
            waiting, power = unpack(PAIR - 1, samp, power)
            for number, (from_side, steps) in enumerate(TURNS):
                peers = [flip(samp, step) for step in steps]
                pair = samp - lax.rem(samp, 2)
                if steps[0] > 1:
                    pair = flip(pair, steps[0])
                if from_side == 0:
                    land_given(pair)
                elif len(steps) == 1:
                    land_lead(peers[0], 1)
                else:
                    land_lead(pair, 2)
                for peer in peers:
                    ahead, power = unpack(from_side, peer, power)
                    totals = multiply(waiting, totals)
                    waiting = ahead
                if all(side == 0 for side, _ in TURNS[number:]) and TURNS[number - 1][0]:
                    message = finish(PAIR - 1, totals, message)
            totals = multiply(waiting, totals)
            message = finish(0, totals, message)
        else:
            ahead, power = unpack(PAIR - 1, samp, power)
            totals = multiply(ahead, totals)
            partner = samp + 1 - 2 * lax.rem(samp, 2)
            land_lead(partner, 1)
            ahead, power = unpack(PAIR - 1, partner, power)
            totals = multiply(ahead, totals)

            def add_lead(step, carry):
                totals, power = carry
                first = 2 * lax.rem(lax.div(samp, 2) + step, samp_size // 2)
                land_lead(first, 2)
                for member in range(2):
                    ahead, power = unpack(PAIR - 1, first + member, power)
                    totals = multiply(ahead, totals)
                return totals, power

            def add_given(two, totals):
                land_given(two * 2)
                for member in range(2):
                    totals = multiply(unpack(0, two * 2 + member, power)[0], totals)
                return totals

            totals, power = lax.fori_loop(1, samp_size // 2, add_lead, (totals, power))
            totals = lax.fori_loop(0, samp_size // 2, add_given, totals)
            for from_side in range(PAIR):
                message = finish(from_side, totals, message)
        squares = lane_sum(jnp.sum(power, axis=0, keepdims=True))
        reports = jnp.logical_and(place == 0, gene == PAIR - 1).astype(jnp.float32)
        message = message + jnp.where(
            (stat_sub == STATS) & (stat_lane >= 0) & (stat_lane < genes), squares * reports, 0.0
        )
        row = jnp.sum(message, axis=0, keepdims=True)

        @pl.when(later > 0)
        def _():
            pl.semaphore_wait(known_sem, samp_size - 1)

        row_out[...] = row
        slot = place * (gene_size // PAIR) + lax.div(gene, PAIR)
        rows[slot] = row

        @pl.loop(0, samp_size)
        def _(samp_to):
            for gene_to in range(gene_size):

                @pl.when(jnp.logical_or(samp_to != samp, gene_to != gene))
                def _(gene_to=gene_to):
                    pltpu.make_async_remote_copy(
                        src_ref=row_out,
                        dst_ref=rows.at[slot],
                        send_sem=send_sem,
                        recv_sem=row_sem,
                        device_id={"samp": samp_to, "gene": gene_to},
                        device_id_type=MESH,
                    ).start()

    @pl.when(owns)
    def _():
        landed = rows.at[pl.ds(0, row_count - 1)]
        pltpu.make_async_copy(landed, landed, row_sem).wait()

    @pl.when(jnp.logical_not(owns))
    def _():
        pltpu.make_async_copy(rows, rows, row_sem).wait()

    totals = jnp.sum(rows[...], axis=0)
    parts = [totals[:, stat * genes : (stat + 1) * genes] for stat in range(STATS + 1)]
    variance = parts[STATS] / (fields * local_rows * samp_size)
    both_ref[0:1] = parts[0] * lax.rsqrt(variance * parts[1])
    both_ref[1:2] = (parts[2] - variance * parts[3]) * lax.rsqrt(2.0 * parts[4]) / variance

    def sent(buffer, count):
        @pl.loop(0, count)
        def _(_):
            pltpu.make_async_copy(buffer, buffer, send_sem).wait()

    sent(tile_out, jnp.where(leads, targets, 0))
    sent(lead_words.at[0], jnp.where(leads, targets, owner_size))
    sent(params.at[0], jnp.where(helps, 1, 0))
    sent(row_out, jnp.where(owns, samp_size * gene_size - 1, 0))


def solution(mesh):
    samp_size, gene_size = mesh.shape["samp"], mesh.shape["gene"]

    def local(
        genotypes, allele_freq, sample_weight, residual, variant_weight, block_gene, gene_variants
    ):
        local_rows, columns = genotypes.shape
        local_blocks = columns // BLK
        fields = sample_weight.shape[0]
        genes = gene_variants.shape[0]
        depth = fields * local_rows // BLK
        width = -(-((STATS + 1) * genes) // BLK) * BLK
        owner_low, owner_size = owner_range(samp_size, local_blocks)
        owned = local_blocks // owner_size
        both = pl.pallas_call(
            functools.partial(kernel, samp_size, gene_size, owner_low, owner_size),
            out_shape=pltpu.VMEM((2, genes), jnp.float32),
            in_specs=[pl.BlockSpec(memory_space=pl.ANY)] * 7,
            out_specs=pl.BlockSpec(memory_space=pltpu.VMEM),
            scratch_shapes=[
                pltpu.VMEM((local_rows, columns), jnp.int32),
                pltpu.VMEM((fields, local_rows), jnp.float32),
                pltpu.VMEM((fields, local_rows), jnp.float32),
                pltpu.VMEM((1, block_gene.shape[0]), jnp.int32),
                pltpu.VMEM((1, genes), jnp.int32),
                pltpu.VMEM((PAIR, 2, local_blocks, BLK), jnp.float32),
                pltpu.VMEM((2 * depth, BLK), jnp.float32),
                pltpu.VMEM((samp_size, 2 * depth, BLK), jnp.float32),
                pltpu.VMEM((samp_size, local_rows, owned * BLK), jnp.int32),
                pltpu.VMEM((samp_size, local_rows, owned * BLK), jnp.int32),
                pltpu.VMEM((PAIR * owned, depth, BLK, BLK), jnp.float32),
                pltpu.VMEM((PAIR * owned, BLK, BLK), jnp.float32),
                pltpu.VMEM((1, width), jnp.float32),
                pltpu.VMEM((owner_size * gene_size // PAIR, 1, width), jnp.float32),
                pltpu.SemaphoreType.DMA((2,)),
                pltpu.SemaphoreType.DMA,
                pltpu.SemaphoreType.DMA((samp_size // 2,)),
                pltpu.SemaphoreType.DMA((samp_size // 2,)),
                pltpu.SemaphoreType.DMA((samp_size // 2,)),
                pltpu.SemaphoreType.DMA,
                pltpu.SemaphoreType.DMA,
                pltpu.SemaphoreType.REGULAR,
                pltpu.SemaphoreType.REGULAR,
            ],
            compiler_params=pltpu.CompilerParams(collective_id=0, has_side_effects=True),
        )(
            genotypes,
            allele_freq.reshape(local_blocks, BLK),
            sample_weight,
            residual,
            variant_weight.reshape(local_blocks, BLK),
            block_gene.reshape(1, -1),
            gene_variants.reshape(1, -1),
        )
        return both[0], both[1]

    placed = (P("samp", "gene"), P("gene"), P(None, "samp"), P(None, "samp"), P("gene"), P(), P())
    return jax.shard_map(local, mesh=mesh, in_specs=placed, out_specs=(P(), P()), check_vma=False)
```

```python
import functools

import jax
import jax.numpy as jnp
from jax import lax
from jax.experimental import pallas as pl
from jax.experimental.pallas import tpu as pltpu
from jax.sharding import PartitionSpec as P

BLK = 128
MESH = pl.DeviceIdType.MESH
STATS = 5
SCORE = 16
PAIR = 2
TURNS = (
    (1, (1,)),
    (0, (0, 1)),
    (1, (4, 5)),
    (1, (6, 7)),
    (0, (4, 5)),
    (1, (2, 3)),
    (0, (6, 7)),
    (0, (2, 3)),
)


def lane_sum(row):
    return jnp.sum(row, axis=1, keepdims=True)


def owner_range(samp_size, local_blocks):
    low = samp_size // 4
    size = max(1, samp_size // 2)
    while local_blocks % size:
        size -= 1
    return low, size


def flip(samp, step):
    peer, bit = samp, 1
    while bit <= step:
        if step & bit:
            peer = peer + bit * (1 - 2 * lax.rem(lax.div(samp, bit), 2))
        bit *= 2
    return peer


def kernel(
    samp_size,
    gene_size,
    owner_low,
    owner_size,
    genotypes_hbm,
    freq_hbm,
    weight_hbm,
    residual_hbm,
    variant_hbm,
    block_gene_hbm,
    counts_hbm,
    both_ref,
    words_in,
    weight_in,
    residual_in,
    block_gene_in,
    counts_in,
    params,
    tile_out,
    tiles,
    lead_words,
    given_words,
    centers,
    pair_weight,
    row_out,
    rows,
    load_sem,
    send_sem,
    tile_sem,
    lead_sem,
    given_sem,
    param_sem,
    row_sem,
    answer_sem,
    known_sem,
):
    samp = lax.axis_index("samp")
    gene = lax.axis_index("gene")
    side = lax.rem(gene, PAIR)
    lead = gene - side + (PAIR - 1)
    fields, local_rows = weight_in.shape
    group = BLK // local_rows
    depth = fields // group
    local_blocks = params.shape[2]
    owned = local_blocks // owner_size
    owner_high = owner_low + owner_size
    genes = counts_in.shape[1]
    width = row_out.shape[1]
    leads = side == PAIR - 1
    in_range = jnp.logical_and(samp >= owner_low, samp < owner_high)
    owns = jnp.logical_and(leads, in_range)
    helps = jnp.logical_and(jnp.logical_not(leads), in_range)
    place = samp - owner_low
    row_count = rows.shape[0]

    loads = [
        pltpu.make_async_copy(source, target, load_sem.at[number])
        for number, source, target in (
            (0, genotypes_hbm, words_in),
            (1, weight_hbm, weight_in),
            (1, residual_hbm, residual_in),
            (1, freq_hbm, params.at[side, 0]),
            (1, variant_hbm, params.at[side, 1]),
            (1, block_gene_hbm, block_gene_in),
            (1, counts_hbm, counts_in),
        )
    ]
    for load in loads:
        load.start()

    def signal(semaphore, samp_to, gene_to):
        pl.semaphore_signal(
            semaphore,
            inc=1,
            device_id={"samp": samp_to, "gene": gene_to},
            device_id_type=MESH,
        )

    barrier = pltpu.get_barrier_semaphore()

    @pl.when(leads)
    def _():
        signal(barrier, samp, gene - 1)

    @pl.when(owns)
    def _():
        @pl.loop(1, samp_size)
        def _(step):
            for other in range(PAIR):
                signal(barrier, lax.rem(samp + step, samp_size), gene - other)

    for gene_to in range(PAIR, gene_size):

        @pl.when(gene_to > lead)
        def _(gene_to=gene_to):
            signal(barrier, samp, gene_to)

    for load in loads[1:]:
        load.wait()
    own_tile = jnp.concatenate(
        [
            jnp.concatenate(
                [part[lanes * depth : (lanes + 1) * depth] for lanes in range(group)], axis=1
            )
            for part in (weight_in[...], residual_in[...])
        ],
        axis=0,
    )
    tile_out[...] = own_tile
    tiles[samp] = own_tile

    targets = jnp.where(in_range, owner_size - 1, owner_size)
    earlier = lead - (PAIR - 1)
    pl.semaphore_wait(barrier, jnp.where(leads, targets, targets + 1) + earlier)

    def tile_copy(owner):
        return pltpu.make_async_remote_copy(
            src_ref=tile_out,
            dst_ref=tiles.at[samp],
            send_sem=send_sem,
            recv_sem=tile_sem.at[lax.div(samp, 2)],
            device_id={"samp": owner, "gene": gene},
            device_id_type=MESH,
        )

    def word_copy(target, semaphore):
        def copy(owner):
            start = pl.multiple_of((owner - owner_low) * (owned * BLK), BLK)
            return pltpu.make_async_remote_copy(
                src_ref=words_in.at[:, pl.ds(start, owned * BLK)],
                dst_ref=target.at[samp],
                send_sem=send_sem,
                recv_sem=semaphore,
                device_id={"samp": owner, "gene": lead},
                device_id_type=MESH,
            )

        return copy

    upward = 2 * samp < 2 * owner_low + owner_size

    def to_owner(send, order, here=False):
        owner = jnp.where(upward, owner_high - 1 - order, owner_low + order)
        if here:
            send(owner).start()
        else:

            @pl.when(owner != samp)
            def _():
                send(owner).start()

    def to_owners(send, here=False):
        for order in range(owner_size):
            to_owner(send, order, here)

    @pl.when(leads)
    def _():
        to_owners(tile_copy)

    loads[0].wait()

    @pl.when(leads)
    def _():
        to_owners(word_copy(lead_words, lead_sem.at[lax.div(samp, 2)]))

    @pl.when(jnp.logical_not(leads))
    def _():
        to_owners(word_copy(given_words, given_sem.at[lax.div(samp, 2)]), True)

    for gene_to in range(gene_size - PAIR):

        @pl.when(gene_to < earlier)
        def _(gene_to=gene_to):
            signal(answer_sem, samp, gene_to)

    later = gene_size - 1 - lead

    @pl.when(helps)
    def _():
        pltpu.make_async_remote_copy(
            src_ref=params.at[0],
            dst_ref=params.at[0],
            send_sem=send_sem,
            recv_sem=param_sem,
            device_id={"samp": samp, "gene": lead},
            device_id_type=MESH,
        ).start()

    @pl.when(later > 0)
    def _():
        pl.semaphore_wait(answer_sem, later)

        @pl.loop(owner_low, owner_high)
        def _(owner):
            @pl.when(jnp.logical_and(owner != samp, leads))
            def _():
                signal(known_sem, owner, gene)

    @pl.when(owns)
    def _():
        pltpu.make_async_copy(params.at[0], params.at[0], param_sem).wait()
        block_gene = block_gene_in[...].astype(jnp.float32)
        counts = counts_in[...].astype(jnp.float32)
        block_lane = lax.broadcasted_iota(jnp.int32, block_gene.shape, 1)
        gene_lane = lax.broadcasted_iota(jnp.int32, counts.shape, 1).astype(jnp.float32)
        column = lax.broadcasted_iota(jnp.int32, (1, BLK), 1).astype(jnp.float32)
        stat_sub = lax.broadcasted_iota(jnp.int32, (8, width), 0)
        stat_lane = lax.broadcasted_iota(jnp.int32, (8, width), 1) - stat_sub * genes
        effective, places = [], []
        for number in range(PAIR * owned):
            from_side, block = divmod(number, owned)
            local_block = place * owned + block
            block_id = (lead - (PAIR - 1) + from_side) * local_blocks + local_block
            gene_of = lane_sum(jnp.where(block_lane == block_id, block_gene, 0.0))
            first = lane_sum(jnp.where(block_gene < gene_of, 1.0, 0.0))
            counted = lane_sum(jnp.where(gene_lane == gene_of, counts, 0.0))
            block_float = jnp.zeros((1, 1), jnp.float32) + block_id.astype(jnp.float32)
            live = (block_float - first) * BLK + column < counted
            weights = jnp.where(live, params[from_side, 1, pl.ds(local_block, 1), :], 0.0)
            effective.append(weights)
            across = jnp.broadcast_to(weights, (BLK, BLK))
            pair_weight[number] = across * across.T
            freq = params[from_side, 0, pl.ds(local_block, 1), :]
            center = 2.0 * jnp.broadcast_to(freq, (BLK, BLK)).T
            for level in range(depth):
                centers[number, level] = center * float(4**level)
            member = stat_lane.astype(jnp.float32) == gene_of
            places.append(jnp.where(member & (stat_sub < STATS), 1.0, 0.0))

        def land(buffer, semaphore):
            pltpu.make_async_copy(buffer, buffer, semaphore).wait()

        def unpack(from_side, peer, power, blocks=tuple(range(owned))):
            tile = tiles[peer]
            weight, resid = tile[:depth], tile[depth:]
            root = jnp.sqrt(weight)
            score = root * resid
            if from_side:
                power = power + weight * resid * resid
            values = []
            buffer = lead_words if from_side else given_words
            for block in blocks:
                part = buffer[peer, :, block * BLK : (block + 1) * BLK]
                turned = jnp.concatenate(
                    [lax.shift_right_logical(part, 2 * depth * lanes) for lanes in range(group)],
                    axis=0,
                ).T
                levels = []
                for level in range(depth):
                    dosage = jnp.bitwise_and(turned, 3 << (2 * level)).astype(jnp.float32)
                    scale = root[level : level + 1] * float(4**-level)
                    center = centers[from_side * owned + block, level]
                    levels.append(((dosage - center) * scale).astype(jnp.bfloat16))
                values.append(jnp.concatenate(levels, axis=1))
            scores = jnp.concatenate(
                [
                    jnp.broadcast_to(score[level : level + 1], (SCORE, BLK)).astype(jnp.bfloat16)
                    for level in range(depth)
                ],
                axis=1,
            )
            return (from_side, blocks, values, scores), power

        def multiply(unpacked, totals):
            from_side, blocks, values, scores = unpacked
            totals = list(totals)
            for value, block in zip(values, blocks):
                number = from_side * owned + block
                totals[number] = totals[number] + lax.dot_general(
                    jnp.concatenate([value, scores], axis=0),
                    value,
                    (((1,), (1,)), ((), ())),
                    preferred_element_type=jnp.float32,
                )
            return tuple(totals)

        own_start = pl.multiple_of(place * (owned * BLK), BLK)
        lead_words[samp] = words_in[:, pl.ds(own_start, owned * BLK)]

        diagonal = lax.broadcasted_iota(jnp.int32, (BLK, BLK), 0) == lax.broadcasted_iota(
            jnp.int32, (BLK, BLK), 1
        )

        def finish(from_side, totals, message):
            for block in range(owned):
                number = from_side * owned + block
                total = totals[number]
                weighted = total[:BLK] * pair_weight[number]
                score = effective[number] * total[BLK : BLK + 1]
                sums = [
                    score,
                    jnp.sum(weighted, axis=0, keepdims=True),
                    score * score,
                    jnp.sum(jnp.where(diagonal, weighted, 0.0), axis=0, keepdims=True),
                    jnp.sum(weighted * weighted, axis=0, keepdims=True),
                    jnp.zeros((8 - STATS, BLK), jnp.float32),
                ]
                message = message + lane_sum(jnp.concatenate(sums, axis=0)) * places[number]
            return message

        def land_lead(first, count):
            two = lax.div(first, 2)
            land(tiles.at[pl.ds(first, count)], tile_sem.at[two])
            land(lead_words.at[pl.ds(first, count)], lead_sem.at[two])

        def land_given(first):
            land(given_words.at[pl.ds(first, 2)], given_sem.at[lax.div(first, 2)])

        message = jnp.zeros((8, width), jnp.float32)
        power = jnp.zeros((depth, BLK), jnp.float32)
        totals = tuple(jnp.zeros((BLK + SCORE, BLK), jnp.float32) for _ in range(PAIR * owned))
        if samp_size == 8:
            waiting, power = unpack(PAIR - 1, samp, power)
            for number, (from_side, steps) in enumerate(TURNS):
                peers = [flip(samp, step) for step in steps]
                pair = samp - lax.rem(samp, 2)
                if steps[0] > 1:
                    pair = flip(pair, steps[0])
                if from_side == 0:
                    land_given(pair)
                elif len(steps) == 1:
                    land_lead(peers[0], 1)
                else:
                    land_lead(pair, 2)
                if number == len(TURNS) - 1:
                    message = finish(PAIR - 1, totals, message)
                if number == len(TURNS) - 1:
                    for block in range(owned):
                        for peer in peers:
                            ahead, power = unpack(from_side, peer, power, (block,))
                            totals = multiply(waiting, totals)
                            waiting = ahead
                    continue
                for peer in peers:
                    ahead, power = unpack(from_side, peer, power)
                    totals = multiply(waiting, totals)
                    waiting = ahead
            totals = multiply(waiting, totals)
            message = finish(0, totals, message)
        else:
            ahead, power = unpack(PAIR - 1, samp, power)
            totals = multiply(ahead, totals)
            partner = samp + 1 - 2 * lax.rem(samp, 2)
            land_lead(partner, 1)
            ahead, power = unpack(PAIR - 1, partner, power)
            totals = multiply(ahead, totals)

            def add_lead(step, carry):
                totals, power = carry
                first = 2 * lax.rem(lax.div(samp, 2) + step, samp_size // 2)
                land_lead(first, 2)
                for member in range(2):
                    ahead, power = unpack(PAIR - 1, first + member, power)
                    totals = multiply(ahead, totals)
                return totals, power

            def add_given(two, totals):
                land_given(two * 2)
                for member in range(2):
                    totals = multiply(unpack(0, two * 2 + member, power)[0], totals)
                return totals

            totals, power = lax.fori_loop(1, samp_size // 2, add_lead, (totals, power))
            totals = lax.fori_loop(0, samp_size // 2, add_given, totals)
            for from_side in range(PAIR):
                message = finish(from_side, totals, message)
        squares = lane_sum(jnp.sum(power, axis=0, keepdims=True))
        reports = jnp.logical_and(place == 0, gene == PAIR - 1).astype(jnp.float32)
        message = message + jnp.where(
            (stat_sub == STATS) & (stat_lane >= 0) & (stat_lane < genes), squares * reports, 0.0
        )
        row = jnp.sum(message, axis=0, keepdims=True)

        @pl.when(later > 0)
        def _():
            pl.semaphore_wait(known_sem, samp_size - 1)

        row_out[...] = row
        slot = place * (gene_size // PAIR) + lax.div(gene, PAIR)
        rows[slot] = row

        @pl.loop(0, samp_size)
        def _(samp_to):
            for gene_to in range(gene_size):

                @pl.when(jnp.logical_or(samp_to != samp, gene_to != gene))
                def _(gene_to=gene_to):
                    pltpu.make_async_remote_copy(
                        src_ref=row_out,
                        dst_ref=rows.at[slot],
                        send_sem=send_sem,
                        recv_sem=row_sem,
                        device_id={"samp": samp_to, "gene": gene_to},
                        device_id_type=MESH,
                    ).start()

    @pl.when(owns)
    def _():
        landed = rows.at[pl.ds(0, row_count - 1)]
        pltpu.make_async_copy(landed, landed, row_sem).wait()

    @pl.when(jnp.logical_not(owns))
    def _():
        pltpu.make_async_copy(rows, rows, row_sem).wait()

    totals = jnp.sum(rows[...], axis=0)
    parts = [totals[:, stat * genes : (stat + 1) * genes] for stat in range(STATS + 1)]
    variance = parts[STATS] / (fields * local_rows * samp_size)
    both_ref[0:1] = parts[0] * lax.rsqrt(variance * parts[1])
    both_ref[1:2] = (parts[2] - variance * parts[3]) * lax.rsqrt(2.0 * parts[4]) / variance

    def sent(buffer, count):
        @pl.loop(0, count)
        def _(_):
            pltpu.make_async_copy(buffer, buffer, send_sem).wait()

    sent(tile_out, jnp.where(leads, targets, 0))
    sent(lead_words.at[0], jnp.where(leads, targets, owner_size))
    sent(params.at[0], jnp.where(helps, 1, 0))
    sent(row_out, jnp.where(owns, samp_size * gene_size - 1, 0))


def solution(mesh):
    samp_size, gene_size = mesh.shape["samp"], mesh.shape["gene"]

    def local(
        genotypes, allele_freq, sample_weight, residual, variant_weight, block_gene, gene_variants
    ):
        local_rows, columns = genotypes.shape
        local_blocks = columns // BLK
        fields = sample_weight.shape[0]
        genes = gene_variants.shape[0]
        depth = fields * local_rows // BLK
        width = -(-((STATS + 1) * genes) // BLK) * BLK
        owner_low, owner_size = owner_range(samp_size, local_blocks)
        owned = local_blocks // owner_size
        both = pl.pallas_call(
            functools.partial(kernel, samp_size, gene_size, owner_low, owner_size),
            out_shape=pltpu.VMEM((2, genes), jnp.float32),
            in_specs=[pl.BlockSpec(memory_space=pl.ANY)] * 7,
            out_specs=pl.BlockSpec(memory_space=pltpu.VMEM),
            scratch_shapes=[
                pltpu.VMEM((local_rows, columns), jnp.int32),
                pltpu.VMEM((fields, local_rows), jnp.float32),
                pltpu.VMEM((fields, local_rows), jnp.float32),
                pltpu.VMEM((1, block_gene.shape[0]), jnp.int32),
                pltpu.VMEM((1, genes), jnp.int32),
                pltpu.VMEM((PAIR, 2, local_blocks, BLK), jnp.float32),
                pltpu.VMEM((2 * depth, BLK), jnp.float32),
                pltpu.VMEM((samp_size, 2 * depth, BLK), jnp.float32),
                pltpu.VMEM((samp_size, local_rows, owned * BLK), jnp.int32),
                pltpu.VMEM((samp_size, local_rows, owned * BLK), jnp.int32),
                pltpu.VMEM((PAIR * owned, depth, BLK, BLK), jnp.float32),
                pltpu.VMEM((PAIR * owned, BLK, BLK), jnp.float32),
                pltpu.VMEM((1, width), jnp.float32),
                pltpu.VMEM((owner_size * gene_size // PAIR, 1, width), jnp.float32),
                pltpu.SemaphoreType.DMA((2,)),
                pltpu.SemaphoreType.DMA,
                pltpu.SemaphoreType.DMA((samp_size // 2,)),
                pltpu.SemaphoreType.DMA((samp_size // 2,)),
                pltpu.SemaphoreType.DMA((samp_size // 2,)),
                pltpu.SemaphoreType.DMA,
                pltpu.SemaphoreType.DMA,
                pltpu.SemaphoreType.REGULAR,
                pltpu.SemaphoreType.REGULAR,
            ],
            compiler_params=pltpu.CompilerParams(collective_id=0, has_side_effects=True),
        )(
            genotypes,
            allele_freq.reshape(local_blocks, BLK),
            sample_weight,
            residual,
            variant_weight.reshape(local_blocks, BLK),
            block_gene.reshape(1, -1),
            gene_variants.reshape(1, -1),
        )
        return both[0], both[1]

    placed = (P("samp", "gene"), P("gene"), P(None, "samp"), P(None, "samp"), P("gene"), P(), P())
    return jax.shard_map(local, mesh=mesh, in_specs=placed, out_specs=(P(), P()), check_vma=False)
```

```python
import functools

import jax
import jax.numpy as jnp
from jax import lax
from jax.experimental import pallas as pl
from jax.experimental.pallas import tpu as pltpu
from jax.sharding import PartitionSpec as P

BLK = 128
MESH = pl.DeviceIdType.MESH
STATS = 5
SCORE = 16
PAIR = 2
TURNS = (
    (1, (1,)),
    (0, (0, 1)),
    (1, (6,)),
    (1, (4,)),
    (1, (7,)),
    (1, (5,)),
    (1, (2,)),
    (0, (4, 5)),
    (1, (3,)),
    (0, (6, 7)),
    (0, (2, 3)),
)


def lane_sum(row):
    return jnp.sum(row, axis=1, keepdims=True)


def owner_range(samp_size, local_blocks):
    low = samp_size // 4
    size = max(1, samp_size // 2)
    while local_blocks % size:
        size -= 1
    return low, size


def flip(samp, step):
    peer, bit = samp, 1
    while bit <= step:
        if step & bit:
            peer = peer + bit * (1 - 2 * lax.rem(lax.div(samp, bit), 2))
        bit *= 2
    return peer


def kernel(
    samp_size,
    gene_size,
    owner_low,
    owner_size,
    genotypes_hbm,
    freq_hbm,
    weight_hbm,
    residual_hbm,
    variant_hbm,
    block_gene_hbm,
    counts_hbm,
    both_ref,
    words_in,
    weight_in,
    residual_in,
    block_gene_in,
    counts_in,
    params,
    tile_out,
    tiles,
    lead_words,
    given_words,
    centers,
    pair_weight,
    row_out,
    rows,
    load_sem,
    send_sem,
    tile_sem,
    lead_sem,
    given_sem,
    param_sem,
    row_sem,
    answer_sem,
    known_sem,
):
    samp = lax.axis_index("samp")
    gene = lax.axis_index("gene")
    side = lax.rem(gene, PAIR)
    lead = gene - side + (PAIR - 1)
    fields, local_rows = weight_in.shape
    group = BLK // local_rows
    depth = fields // group
    local_blocks = params.shape[2]
    owned = local_blocks // owner_size
    owner_high = owner_low + owner_size
    genes = counts_in.shape[1]
    width = row_out.shape[1]
    leads = side == PAIR - 1
    in_range = jnp.logical_and(samp >= owner_low, samp < owner_high)
    owns = jnp.logical_and(leads, in_range)
    helps = jnp.logical_and(jnp.logical_not(leads), in_range)
    place = samp - owner_low
    row_count = rows.shape[0]

    loads = [
        pltpu.make_async_copy(source, target, load_sem.at[number])
        for number, source, target in (
            (0, genotypes_hbm, words_in),
            (1, weight_hbm, weight_in),
            (1, residual_hbm, residual_in),
            (1, freq_hbm, params.at[side, 0]),
            (1, variant_hbm, params.at[side, 1]),
            (1, block_gene_hbm, block_gene_in),
            (1, counts_hbm, counts_in),
        )
    ]
    for load in loads:
        load.start()

    def signal(semaphore, samp_to, gene_to):
        pl.semaphore_signal(
            semaphore,
            inc=1,
            device_id={"samp": samp_to, "gene": gene_to},
            device_id_type=MESH,
        )

    barrier = pltpu.get_barrier_semaphore()

    @pl.when(leads)
    def _():
        signal(barrier, samp, gene - 1)

    @pl.when(owns)
    def _():
        @pl.loop(1, samp_size)
        def _(step):
            for other in range(PAIR):
                signal(barrier, lax.rem(samp + step, samp_size), gene - other)

    for gene_to in range(PAIR, gene_size):

        @pl.when(gene_to > lead)
        def _(gene_to=gene_to):
            signal(barrier, samp, gene_to)

    for load in loads[1:]:
        load.wait()
    own_tile = jnp.concatenate(
        [
            jnp.concatenate(
                [part[lanes * depth : (lanes + 1) * depth] for lanes in range(group)], axis=1
            )
            for part in (weight_in[...], residual_in[...])
        ],
        axis=0,
    )
    tile_out[...] = own_tile
    tiles[samp] = own_tile

    targets = jnp.where(in_range, owner_size - 1, owner_size)
    earlier = lead - (PAIR - 1)
    pl.semaphore_wait(barrier, jnp.where(leads, targets, targets + 1) + earlier)

    def tile_copy(owner):
        return pltpu.make_async_remote_copy(
            src_ref=tile_out,
            dst_ref=tiles.at[samp],
            send_sem=send_sem,
            recv_sem=tile_sem.at[lax.div(samp, 2)],
            device_id={"samp": owner, "gene": gene},
            device_id_type=MESH,
        )

    def word_copy(target, semaphore):
        def copy(owner):
            start = pl.multiple_of((owner - owner_low) * (owned * BLK), BLK)
            return pltpu.make_async_remote_copy(
                src_ref=words_in.at[:, pl.ds(start, owned * BLK)],
                dst_ref=target.at[samp],
                send_sem=send_sem,
                recv_sem=semaphore,
                device_id={"samp": owner, "gene": lead},
                device_id_type=MESH,
            )

        return copy

    upward = 2 * samp < 2 * owner_low + owner_size

    def to_owner(send, order, here=False):
        owner = jnp.where(upward, owner_high - 1 - order, owner_low + order)
        if here:
            send(owner).start()
        else:

            @pl.when(owner != samp)
            def _():
                send(owner).start()

    def to_owners(send, here=False):
        for order in range(owner_size):
            to_owner(send, order, here)

    @pl.when(leads)
    def _():
        to_owners(tile_copy)

    loads[0].wait()

    @pl.when(leads)
    def _():
        to_owners(word_copy(lead_words, lead_sem.at[samp]))

    @pl.when(jnp.logical_not(leads))
    def _():
        to_owners(word_copy(given_words, given_sem.at[lax.div(samp, 2)]), True)

    for gene_to in range(gene_size - PAIR):

        @pl.when(gene_to < earlier)
        def _(gene_to=gene_to):
            signal(answer_sem, samp, gene_to)

    later = gene_size - 1 - lead

    @pl.when(helps)
    def _():
        pltpu.make_async_remote_copy(
            src_ref=params.at[0],
            dst_ref=params.at[0],
            send_sem=send_sem,
            recv_sem=param_sem,
            device_id={"samp": samp, "gene": lead},
            device_id_type=MESH,
        ).start()

    @pl.when(later > 0)
    def _():
        pl.semaphore_wait(answer_sem, later)

        @pl.loop(owner_low, owner_high)
        def _(owner):
            @pl.when(jnp.logical_and(owner != samp, leads))
            def _():
                signal(known_sem, owner, gene)

    @pl.when(owns)
    def _():
        pltpu.make_async_copy(params.at[0], params.at[0], param_sem).wait()
        block_gene = block_gene_in[...].astype(jnp.float32)
        counts = counts_in[...].astype(jnp.float32)
        block_lane = lax.broadcasted_iota(jnp.int32, block_gene.shape, 1)
        gene_lane = lax.broadcasted_iota(jnp.int32, counts.shape, 1).astype(jnp.float32)
        column = lax.broadcasted_iota(jnp.int32, (1, BLK), 1).astype(jnp.float32)
        stat_sub = lax.broadcasted_iota(jnp.int32, (8, width), 0)
        stat_lane = lax.broadcasted_iota(jnp.int32, (8, width), 1) - stat_sub * genes
        effective, places = [], []
        for number in range(PAIR * owned):
            from_side, block = divmod(number, owned)
            local_block = place * owned + block
            block_id = (lead - (PAIR - 1) + from_side) * local_blocks + local_block
            gene_of = lane_sum(jnp.where(block_lane == block_id, block_gene, 0.0))
            first = lane_sum(jnp.where(block_gene < gene_of, 1.0, 0.0))
            counted = lane_sum(jnp.where(gene_lane == gene_of, counts, 0.0))
            block_float = jnp.zeros((1, 1), jnp.float32) + block_id.astype(jnp.float32)
            live = (block_float - first) * BLK + column < counted
            weights = jnp.where(live, params[from_side, 1, pl.ds(local_block, 1), :], 0.0)
            effective.append(weights)
            across = jnp.broadcast_to(weights, (BLK, BLK))
            pair_weight[number] = across * across.T
            freq = params[from_side, 0, pl.ds(local_block, 1), :]
            center = 2.0 * jnp.broadcast_to(freq, (BLK, BLK)).T
            for level in range(depth):
                centers[number, level] = center * float(4**level)
            member = stat_lane.astype(jnp.float32) == gene_of
            places.append(jnp.where(member & (stat_sub < STATS), 1.0, 0.0))

        def land(buffer, semaphore):
            pltpu.make_async_copy(buffer, buffer, semaphore).wait()

        def unpack(from_side, peer, power, blocks=tuple(range(owned))):
            tile = tiles[peer]
            weight, resid = tile[:depth], tile[depth:]
            root = jnp.sqrt(weight)
            score = root * resid
            if from_side:
                power = power + weight * resid * resid
            values = []
            buffer = lead_words if from_side else given_words
            for block in blocks:
                part = buffer[peer, :, block * BLK : (block + 1) * BLK]
                turned = jnp.concatenate(
                    [lax.shift_right_logical(part, 2 * depth * lanes) for lanes in range(group)],
                    axis=0,
                ).T
                levels = []
                for level in range(depth):
                    dosage = jnp.bitwise_and(turned, 3 << (2 * level)).astype(jnp.float32)
                    scale = root[level : level + 1] * float(4**-level)
                    center = centers[from_side * owned + block, level]
                    levels.append(((dosage - center) * scale).astype(jnp.bfloat16))
                values.append(jnp.concatenate(levels, axis=1))
            scores = jnp.concatenate(
                [
                    jnp.broadcast_to(score[level : level + 1], (SCORE, BLK)).astype(jnp.bfloat16)
                    for level in range(depth)
                ],
                axis=1,
            )
            return (from_side, blocks, values, scores), power

        def multiply(unpacked, totals):
            from_side, blocks, values, scores = unpacked
            totals = list(totals)
            for value, block in zip(values, blocks):
                number = from_side * owned + block
                totals[number] = totals[number] + lax.dot_general(
                    jnp.concatenate([value, scores], axis=0),
                    value,
                    (((1,), (1,)), ((), ())),
                    preferred_element_type=jnp.float32,
                )
            return tuple(totals)

        own_start = pl.multiple_of(place * (owned * BLK), BLK)
        lead_words[samp] = words_in[:, pl.ds(own_start, owned * BLK)]

        diagonal = lax.broadcasted_iota(jnp.int32, (BLK, BLK), 0) == lax.broadcasted_iota(
            jnp.int32, (BLK, BLK), 1
        )

        def finish(from_side, totals, message):
            for block in range(owned):
                number = from_side * owned + block
                total = totals[number]
                weighted = total[:BLK] * pair_weight[number]
                score = effective[number] * total[BLK : BLK + 1]
                sums = [
                    score,
                    jnp.sum(weighted, axis=0, keepdims=True),
                    score * score,
                    jnp.sum(jnp.where(diagonal, weighted, 0.0), axis=0, keepdims=True),
                    jnp.sum(weighted * weighted, axis=0, keepdims=True),
                    jnp.zeros((8 - STATS, BLK), jnp.float32),
                ]
                message = message + lane_sum(jnp.concatenate(sums, axis=0)) * places[number]
            return message

        def land_tiles(first, count):
            land(tiles.at[pl.ds(first, count)], tile_sem.at[lax.div(first, 2)])

        def land_lead(peer):
            land(lead_words.at[peer], lead_sem.at[peer])

        def land_given(first):
            land(given_words.at[pl.ds(first, 2)], given_sem.at[lax.div(first, 2)])

        message = jnp.zeros((8, width), jnp.float32)
        power = jnp.zeros((depth, BLK), jnp.float32)
        totals = tuple(jnp.zeros((BLK + SCORE, BLK), jnp.float32) for _ in range(PAIR * owned))
        if samp_size == 8:
            waiting, power = unpack(PAIR - 1, samp, power)
            for number, (from_side, steps) in enumerate(TURNS):
                peers = [flip(samp, step) for step in steps]
                pair = samp - lax.rem(samp, 2)
                if steps[0] > 1:
                    pair = flip(pair, steps[0] - steps[0] % 2)
                if from_side == 0:
                    land_given(pair)
                else:
                    if steps[0] == 1:
                        land_tiles(peers[0], 1)
                    elif steps[0] % 2 == 0:
                        land_tiles(pair, 2)
                    for peer in peers:
                        land_lead(peer)
                if number == len(TURNS) - 1:
                    message = finish(PAIR - 1, totals, message)
                if number == len(TURNS) - 1:
                    for block in range(owned):
                        for peer in peers:
                            ahead, power = unpack(from_side, peer, power, (block,))
                            totals = multiply(waiting, totals)
                            waiting = ahead
                    continue
                for peer in peers:
                    ahead, power = unpack(from_side, peer, power)
                    totals = multiply(waiting, totals)
                    waiting = ahead
            totals = multiply(waiting, totals)
            message = finish(0, totals, message)
        else:
            ahead, power = unpack(PAIR - 1, samp, power)
            totals = multiply(ahead, totals)
            partner = samp + 1 - 2 * lax.rem(samp, 2)
            land_tiles(partner, 1)
            land_lead(partner)
            ahead, power = unpack(PAIR - 1, partner, power)
            totals = multiply(ahead, totals)

            def add_lead(step, carry):
                totals, power = carry
                first = 2 * lax.rem(lax.div(samp, 2) + step, samp_size // 2)
                land_tiles(first, 2)
                land_lead(first)
                land_lead(first + 1)
                for member in range(2):
                    ahead, power = unpack(PAIR - 1, first + member, power)
                    totals = multiply(ahead, totals)
                return totals, power

            def add_given(two, totals):
                land_given(two * 2)
                for member in range(2):
                    totals = multiply(unpack(0, two * 2 + member, power)[0], totals)
                return totals

            totals, power = lax.fori_loop(1, samp_size // 2, add_lead, (totals, power))
            totals = lax.fori_loop(0, samp_size // 2, add_given, totals)
            for from_side in range(PAIR):
                message = finish(from_side, totals, message)
        squares = lane_sum(jnp.sum(power, axis=0, keepdims=True))
        reports = jnp.logical_and(place == 0, gene == PAIR - 1).astype(jnp.float32)
        message = message + jnp.where(
            (stat_sub == STATS) & (stat_lane >= 0) & (stat_lane < genes), squares * reports, 0.0
        )
        row = jnp.sum(message, axis=0, keepdims=True)

        @pl.when(later > 0)
        def _():
            pl.semaphore_wait(known_sem, samp_size - 1)

        row_out[...] = row
        slot = place * (gene_size // PAIR) + lax.div(gene, PAIR)
        rows[slot] = row

        @pl.loop(0, samp_size)
        def _(samp_to):
            for gene_to in range(gene_size):

                @pl.when(jnp.logical_or(samp_to != samp, gene_to != gene))
                def _(gene_to=gene_to):
                    pltpu.make_async_remote_copy(
                        src_ref=row_out,
                        dst_ref=rows.at[slot],
                        send_sem=send_sem,
                        recv_sem=row_sem,
                        device_id={"samp": samp_to, "gene": gene_to},
                        device_id_type=MESH,
                    ).start()

    @pl.when(owns)
    def _():
        landed = rows.at[pl.ds(0, row_count - 1)]
        pltpu.make_async_copy(landed, landed, row_sem).wait()

    @pl.when(jnp.logical_not(owns))
    def _():
        pltpu.make_async_copy(rows, rows, row_sem).wait()

    totals = jnp.sum(rows[...], axis=0)
    parts = [totals[:, stat * genes : (stat + 1) * genes] for stat in range(STATS + 1)]
    variance = parts[STATS] / (fields * local_rows * samp_size)
    both_ref[0:1] = parts[0] * lax.rsqrt(variance * parts[1])
    both_ref[1:2] = (parts[2] - variance * parts[3]) * lax.rsqrt(2.0 * parts[4]) / variance

    def sent(buffer, count):
        @pl.loop(0, count)
        def _(_):
            pltpu.make_async_copy(buffer, buffer, send_sem).wait()

    sent(tile_out, jnp.where(leads, targets, 0))
    sent(lead_words.at[0], jnp.where(leads, targets, owner_size))
    sent(params.at[0], jnp.where(helps, 1, 0))
    sent(row_out, jnp.where(owns, samp_size * gene_size - 1, 0))


def solution(mesh):
    samp_size, gene_size = mesh.shape["samp"], mesh.shape["gene"]

    def local(
        genotypes, allele_freq, sample_weight, residual, variant_weight, block_gene, gene_variants
    ):
        local_rows, columns = genotypes.shape
        local_blocks = columns // BLK
        fields = sample_weight.shape[0]
        genes = gene_variants.shape[0]
        depth = fields * local_rows // BLK
        width = -(-((STATS + 1) * genes) // BLK) * BLK
        owner_low, owner_size = owner_range(samp_size, local_blocks)
        owned = local_blocks // owner_size
        both = pl.pallas_call(
            functools.partial(kernel, samp_size, gene_size, owner_low, owner_size),
            out_shape=pltpu.VMEM((2, genes), jnp.float32),
            in_specs=[pl.BlockSpec(memory_space=pl.ANY)] * 7,
            out_specs=pl.BlockSpec(memory_space=pltpu.VMEM),
            scratch_shapes=[
                pltpu.VMEM((local_rows, columns), jnp.int32),
                pltpu.VMEM((fields, local_rows), jnp.float32),
                pltpu.VMEM((fields, local_rows), jnp.float32),
                pltpu.VMEM((1, block_gene.shape[0]), jnp.int32),
                pltpu.VMEM((1, genes), jnp.int32),
                pltpu.VMEM((PAIR, 2, local_blocks, BLK), jnp.float32),
                pltpu.VMEM((2 * depth, BLK), jnp.float32),
                pltpu.VMEM((samp_size, 2 * depth, BLK), jnp.float32),
                pltpu.VMEM((samp_size, local_rows, owned * BLK), jnp.int32),
                pltpu.VMEM((samp_size, local_rows, owned * BLK), jnp.int32),
                pltpu.VMEM((PAIR * owned, depth, BLK, BLK), jnp.float32),
                pltpu.VMEM((PAIR * owned, BLK, BLK), jnp.float32),
                pltpu.VMEM((1, width), jnp.float32),
                pltpu.VMEM((owner_size * gene_size // PAIR, 1, width), jnp.float32),
                pltpu.SemaphoreType.DMA((2,)),
                pltpu.SemaphoreType.DMA,
                pltpu.SemaphoreType.DMA((samp_size // 2,)),
                pltpu.SemaphoreType.DMA((samp_size,)),
                pltpu.SemaphoreType.DMA((samp_size // 2,)),
                pltpu.SemaphoreType.DMA,
                pltpu.SemaphoreType.DMA,
                pltpu.SemaphoreType.REGULAR,
                pltpu.SemaphoreType.REGULAR,
            ],
            compiler_params=pltpu.CompilerParams(collective_id=0, has_side_effects=True),
        )(
            genotypes,
            allele_freq.reshape(local_blocks, BLK),
            sample_weight,
            residual,
            variant_weight.reshape(local_blocks, BLK),
            block_gene.reshape(1, -1),
            gene_variants.reshape(1, -1),
        )
        return both[0], both[1]

    placed = (P("samp", "gene"), P("gene"), P(None, "samp"), P(None, "samp"), P("gene"), P(), P())
    return jax.shard_map(local, mesh=mesh, in_specs=placed, out_specs=(P(), P()), check_vma=False)
```
